32 devices in a mesh: section: 4 (over y, x), dev: 8 (over z, core).
Axes of the slice: x: 2, y: 2, z: 4, core: 2. Of those that a mesh axis runs over, the one named last changes fastest.
Arguments:
- late_sent: bfloat16 [4, 784, 1024], P('section', 'dev'), may hold values from -5 to 5
- entry_rows: bfloat16 [784, 1024], P('dev'), may hold values from -5 to 5
- gain_first: float32 [4, 1024], P('section'), may hold values from 0.1 to 1.9
- shift_first: float32 [4, 1024], P('section'), may hold values from -3 to 3
- expand_late: bfloat16 [4, 1024, 4096], P('section', None, 'dev'), may hold values from -0.1875 to 0.1875
- gain_inner: float32 [4, 4096], P('section', 'dev'), may hold values from 0.1 to 1.9
- shift_inner: float32 [4, 4096], P('section', 'dev'), may hold values from -3 to 3
- reduce_late: bfloat16 [4, 4096, 1024], P('section', 'dev'), may hold values from -0.09375 to 0.09375
- early_saved: bfloat16 [4, 12544, 256], P('section', 'dev'), may hold values from -6 to 6
- upstream_grad: bfloat16 [4, 12544, 256], P('section', 'dev'), may hold values from -6 to 6
- exit_grad: bfloat16 [12544, 256], P('dev'), may hold values from -6 to 6
- expand_early: bfloat16 [4, 256, 1024], P('section'), may hold values from -0.375 to 0.375
- reduce_early: bfloat16 [4, 1024, 256], P('section'), may hold values from -0.1875 to 0.1875
Outputs:
- late_out: bfloat16 [4, 784, 1024], P('section', 'dev')
- input_grad: bfloat16 [4, 12544, 256], P('section', 'dev')
- grad_expand: float32 [4, 256, 1024], P('section')
- grad_reduce: float32 [4, 1024, 256], P('section')
The draws below stay inside these ranges and needn't reach their ends.
All inputs are finite; a program needn't handle non-finite values.
Results may differ from the reference program's by a relative error of at most 0.02.
Values may be sent and summed in bfloat16 or wider, within the bound.
No kernel may reach another device: no remote copies, remote signals or barrier semaphores. Data moves between devices by JAX's collectives and lax.ppermute only.
A program may use at most 128 MiB of HBM per device.

```python
import math
import jax
import jax.numpy as jnp
from jax import lax

CE = 256
FE = 1024
CL = 1024
FL = 4096
SECTIONS = 4
HID_DEV = 512
E_ROWS = 12544
L_ROWS = 784
N_DEV = 8


def scaled_rows(key, leading):
    keys = jax.random.split(key, 4)
    shape = (leading, L_ROWS, CL)
    base = jnp.clip(jax.random.normal(keys[0], shape, jnp.float32), -4.0, 4.0)
    weight = 0.5
    rise = 6.0
    trend = jnp.exp(math.log(rise) * jnp.arange(L_ROWS, dtype=jnp.float32) / L_ROWS).reshape(1, L_ROWS, 1)
    row_factor = jnp.exp(jax.random.uniform(keys[1], (leading, L_ROWS, 1), jnp.float32, 0.0, math.log(2.0)))
    column_factor = jnp.exp(jax.random.uniform(keys[2], (leading, 1, CL), jnp.float32, 0.0, math.log(10.0)))
    offset = jnp.clip(jax.random.normal(keys[3], (leading, 1, CL), jnp.float32), -2.0, 2.0) * weight
    return 0.005 * (base * row_factor + offset) * trend * column_factor


def draw_late_sent(key, part):
    return scaled_rows(jax.random.fold_in(key, 101), SECTIONS).astype(jnp.bfloat16)


def draw_entry_rows(key, part):
    return scaled_rows(jax.random.fold_in(key, 202), 1)[0].astype(jnp.bfloat16)


def block_scale(own_key, shape, shards, smallest, top_value):
    loudness = 1.0
    for position, parts in shards:
        steps = jax.random.uniform(jax.random.fold_in(jax.random.fold_in(own_key, 6), position), (parts,), jnp.float32, smallest / len(shards), top_value / len(shards))
        loudness = loudness * jnp.repeat(jnp.exp(steps), shape[position] // parts).reshape((-1,) + (1,) * (len(shape) - 1 - position))
    return loudness


def scatter_about(own_key, extent, deviation, reach, cuts=(), held_as=jnp.bfloat16):
    values = jax.random.normal(own_key, extent, jnp.float32) * deviation
    if len(cuts) > 0:
        values = block_scale(own_key, extent, cuts, -0.22, 0.18) * values
    return jnp.clip(values, min=-reach, max=reach).astype(held_as)


def setup_inputs(seed: int = 0) -> dict:
    key_of = jax.random.split(jax.random.key(seed), 14)
    return {
        "late_sent": draw_late_sent(jax.random.fold_in(key_of[13], 71), 0),
        "entry_rows": draw_entry_rows(jax.random.fold_in(key_of[13], 71), 0),
        "gain_first": jnp.clip(1.0 + 0.18 * jax.random.normal(key_of[2], (SECTIONS, CL), jnp.float32), 0.1, 1.9),
        "shift_first": scatter_about(key_of[3], (SECTIONS, CL), 0.5, 3.0, ((0, 4),), jnp.float32),
        "expand_late": scatter_about(key_of[4], (SECTIONS, CL, FL), CL ** -0.5, 0.1875, ((0, 4), (2, 8))),
        "gain_inner": jnp.clip(1.0 + 0.18 * jax.random.normal(key_of[5], (SECTIONS, FL), jnp.float32), 0.1, 1.9),
        "shift_inner": scatter_about(key_of[6], (SECTIONS, FL), 0.5, 3.0, ((0, 4), (1, 8)), jnp.float32),
        "reduce_late": scatter_about(key_of[7], (SECTIONS, FL, CL), FL ** -0.5, 0.09375, ((0, 4), (1, 8))),
        "early_saved": scatter_about(key_of[8], (SECTIONS, E_ROWS, CE), 1.0, 6.0, ((0, 4), (1, 8))),
        "upstream_grad": scatter_about(key_of[9], (SECTIONS, E_ROWS, CE), 1.0, 6.0, ((0, 4), (1, 8))),
        "exit_grad": scatter_about(key_of[10], (E_ROWS, CE), 1.0, 6.0, ((0, 8),)),
        "expand_early": scatter_about(key_of[11], (SECTIONS, CE, FE), CE ** -0.5, 0.375, ((0, 4),)),
        "reduce_early": scatter_about(key_of[12], (SECTIONS, FE, CE), FE ** -0.5, 0.1875, ((0, 4),)),
    }


epsilon = 1e-05

def affine(sums, squares, count, gain, shift):
    average = sums / count
    second = squares / count
    spread = gain * lax.rsqrt(second - average * average + epsilon)
    return (spread, shift - average * spread)

def silu_slope(values):
    sigma = jax.nn.sigmoid(values)
    return sigma * (1.0 + values * (1.0 - sigma))

def late_block(inputs, gain_first, shift_first, expand, gain_inner, shift_inner, reduce_weight):
    count = inputs.shape[0]
    values = inputs.astype(jnp.float32)
    spread, offset = affine(lax.optimization_barrier(jnp.sum(values, axis=0)), lax.optimization_barrier(jnp.sum(values * values, axis=0)), count, gain_first, shift_first)
    first = jax.nn.silu(values * spread + offset).astype(jnp.bfloat16)
    inner = jnp.dot(first, expand, preferred_element_type=jnp.float32)
    spread_two, offset_two = affine(lax.optimization_barrier(jnp.sum(inner, axis=0)), lax.optimization_barrier(jnp.sum(inner * inner, axis=0)), count, gain_inner, shift_inner)
    hidden = jax.nn.silu(inner * spread_two + offset_two).astype(jnp.bfloat16)

    def add_group(total, group):
        start = (group * HID_DEV).astype(jnp.int32)
        term = jnp.dot(lax.dynamic_slice_in_dim(hidden, start, HID_DEV, 1), lax.dynamic_slice_in_dim(reduce_weight, start, HID_DEV, 0), preferred_element_type=jnp.float32)
        rounded = lax.optimization_barrier(term.astype(jnp.bfloat16))
        return (total + rounded.astype(jnp.float32), None)
    total, unused = lax.scan(add_group, jnp.zeros((count, CL), jnp.float32), jnp.arange(N_DEV, dtype=jnp.int32))
    return (values + total).astype(jnp.bfloat16)

def early_block(saved, grad, expand, reduce_weight):
    pre = jnp.dot(saved, expand, preferred_element_type=jnp.float32)
    hidden = jax.nn.silu(pre).astype(jnp.bfloat16)
    back = lax.dot_general(grad, reduce_weight, (((1,), (1,)), ((), ())), preferred_element_type=jnp.float32)
    slope = (back * silu_slope(pre)).astype(jnp.bfloat16)
    result = grad.astype(jnp.float32) + lax.dot_general(slope, expand, (((1,), (1,)), ((), ())), preferred_element_type=jnp.float32)
    grad_expand = lax.dot_general(saved, slope, (((0,), (0,)), ((), ())), preferred_element_type=jnp.float32)
    grad_reduce = lax.dot_general(hidden, grad, (((0,), (0,)), ((), ())), preferred_element_type=jnp.float32)
    return (result.astype(jnp.bfloat16), grad_expand, grad_reduce)

def reference(late_sent, entry_rows, gain_first, shift_first, expand_late, gain_inner, shift_inner, reduce_late, early_saved, upstream_grad, exit_grad, expand_early, reduce_early):
    late_in = jnp.concatenate([entry_rows[None], late_sent[:-1]], axis=0)
    grad_in = jnp.concatenate([upstream_grad[1:], exit_grad[None]], axis=0)
    late_out = lax.map(lambda items: late_block(*items), (late_in, gain_first, shift_first, expand_late, gain_inner, shift_inner, reduce_late))
    input_grad, grad_expand, grad_reduce = lax.map(lambda items: early_block(*items), (early_saved, grad_in, expand_early, reduce_early))
    factor = 1.0 / math.sqrt(E_ROWS)
    return (late_out, input_grad, grad_expand * factor, grad_reduce * factor)
```

```python
import math

import jax
import jax.numpy as jnp
from jax import lax
from jax.sharding import PartitionSpec as P

epsilon = 1e-05
bf16 = jnp.bfloat16
f32 = jnp.float32


def from_behind(x, axis, by):
    peers = lax.axis_size(axis)
    pairs = [(i, i + by) for i in range(peers) if 0 <= i + by < peers]
    return lax.ppermute(x, axis, pairs)


def swap(x):
    return lax.ppermute(x, "dev", [(i, i ^ 1) for i in range(lax.axis_size("dev"))])


def chips():
    return lax.axis_size("dev") // 2


def partner(chip, step):
    count = chips()
    return chip ^ step if count & (count - 1) == 0 else (chip + step) % count


def across(x, step, back=False):
    pairs = []
    for chip in range(chips()):
        for core in range(2):
            here, there = 2 * chip + core, 2 * partner(chip, step) + core
            pairs.append((there, here) if back else (here, there))
    return lax.ppermute(x, "dev", pairs)


def steps_far_first():
    return list(range(chips() - 1, 0, -1))


def affine(sums, squares, count, gain, shift):
    average = sums / count
    second = squares / count
    spread = gain * lax.rsqrt(second - average * average + epsilon)
    return (spread, shift - average * spread)


def silu_slope(values):
    sigma = jax.nn.sigmoid(values)
    return sigma * (1.0 + values * (1.0 - sigma))


def late_part(
    late_sent,
    entry_rows,
    gain_first,
    shift_first,
    expand_late,
    gain_inner,
    shift_inner,
    reduce_late,
):
    section_index = lax.axis_index("section")
    total_rows = entry_rows.shape[0] * lax.axis_size("dev")
    arrived = from_behind(late_sent[0], "section", 1)
    expand, reduce_weight = expand_late[0], reduce_late[0]
    expand_two, reduce_two = swap(expand), swap(reduce_weight)
    inner_affine = jnp.concatenate([gain_inner, shift_inner], axis=0)
    affine_two = swap(inner_affine)
    own_rows = jnp.where(section_index == 0, entry_rows, arrived)
    blocks = {0: own_rows}
    for step in steps_far_first():
        blocks[step] = across(own_rows, step, back=True)
    rows = jnp.stack([blocks[step] for step in range(chips())])
    values = rows.astype(f32)
    mine = jnp.stack([jnp.sum(values, axis=(0, 1)), jnp.sum(values * values, axis=(0, 1))])
    total = mine + swap(mine)
    spread, offset = affine(total[0], total[1], total_rows, gain_first[0], shift_first[0])
    first = jax.nn.silu(values * spread + offset).astype(bf16)

    def expanded(weight):
        inner = lax.dot_general(first, weight, (((2,), (0,)), ((), ())), preferred_element_type=f32)
        return inner, jnp.stack([jnp.sum(inner, axis=(0, 1)), jnp.sum(inner * inner, axis=(0, 1))])

    inner_one, sums_one = expanded(expand)
    inner_two, sums_two = expanded(expand_two)
    got = swap(jnp.stack([sums_two, sums_one]))
    total_one, total_two = sums_one + got[0], sums_two + got[1]

    def hidden_of(inner, total, gain_shift):
        spread_two, offset_two = affine(total[0], total[1], total_rows, gain_shift[0], gain_shift[1])
        return jax.nn.silu(inner * spread_two + offset_two).astype(bf16)

    hidden_one = hidden_of(inner_one, total_one, inner_affine)
    hidden_two = hidden_of(inner_two, total_two, affine_two)

    def reduced(step):
        return jnp.dot(hidden_one[step], reduce_weight, preferred_element_type=f32) + jnp.dot(
            hidden_two[step], reduce_two, preferred_element_type=f32
        )

    result = own_rows.astype(f32) + reduced(0)
    for step in steps_far_first():
        result = result + across(reduced(step).astype(bf16), step).astype(f32)
    return result.astype(bf16)[None]


def summed_over_dev(terms, factor):
    count = chips()
    device = lax.axis_index("dev")
    chip, core = device // 2, device % 2
    halves = []
    for term in terms:
        part = term.reshape(2, term.shape[0] // 2, term.shape[1])
        keep = lax.dynamic_index_in_dim(part, core, 0, keepdims=False)
        send = lax.dynamic_index_in_dim(part, 1 - core, 0, keepdims=False).astype(bf16)
        halves.append(keep + swap(send).astype(f32))
    shares = []
    for half in halves:
        pieces = half.reshape(count, half.shape[0] // count, half.shape[1])
        shares.append(pieces)
    sums = [lax.dynamic_index_in_dim(pieces, chip, 0, keepdims=False) for pieces in shares]
    for step in steps_far_first():
        for index, pieces in enumerate(shares):
            piece = lax.dynamic_index_in_dim(pieces, partner(chip, step), 0, keepdims=False)
            sums[index] = sums[index] + across(piece.astype(bf16), step).astype(f32)
    results = []
    for term, total in zip(terms, sums):
        own = (total * factor).astype(bf16)
        gathered = jnp.zeros((count,) + own.shape, bf16)
        gathered = lax.dynamic_update_index_in_dim(gathered, own, chip, 0)
        for step in steps_far_first():
            gathered = lax.dynamic_update_index_in_dim(
                gathered, across(own, step, back=True), partner(chip, step), 0
            )
        half = gathered.reshape(term.shape[0] // 2, term.shape[1])
        other = swap(half)
        both = jnp.where(core == 0, jnp.stack([half, other]), jnp.stack([other, half]))
        results.append(both.reshape(term.shape).astype(f32))
    return results


def early_part(early_saved, upstream_grad, exit_grad, expand_early, reduce_early):
    section_index = lax.axis_index("section")
    arrived = from_behind(upstream_grad[0], "section", -1)
    grad = jnp.where(section_index == lax.axis_size("section") - 1, exit_grad, arrived)
    saved = early_saved[0]
    expand = expand_early[0]
    reduce_weight = reduce_early[0]
    pre = jnp.dot(saved, expand, preferred_element_type=f32)
    hidden = jax.nn.silu(pre).astype(bf16)
    back = lax.dot_general(grad, reduce_weight, (((1,), (1,)), ((), ())), preferred_element_type=f32)
    slope = (back * silu_slope(pre)).astype(bf16)
    local_expand = lax.dot_general(
        saved, slope, (((0,), (0,)), ((), ())), preferred_element_type=f32
    )
    local_reduce = lax.dot_general(
        hidden, grad, (((0,), (0,)), ((), ())), preferred_element_type=f32
    )
    factor = 1.0 / math.sqrt(saved.shape[0] * lax.axis_size("dev"))
    sum_expand, sum_reduce = summed_over_dev((local_expand, local_reduce), factor)
    result = grad.astype(f32) + lax.dot_general(
        slope, expand, (((1,), (1,)), ((), ())), preferred_element_type=f32
    )
    return (result.astype(bf16)[None], sum_expand[None], sum_reduce[None])


def shards(
    late_sent,
    entry_rows,
    gain_first,
    shift_first,
    expand_late,
    gain_inner,
    shift_inner,
    reduce_late,
    early_saved,
    upstream_grad,
    exit_grad,
    expand_early,
    reduce_early,
):
    late_out = late_part(
        late_sent,
        entry_rows,
        gain_first,
        shift_first,
        expand_late,
        gain_inner,
        shift_inner,
        reduce_late,
    )
    input_grad, grad_expand, grad_reduce = early_part(
        early_saved, upstream_grad, exit_grad, expand_early, reduce_early
    )
    return (late_out, input_grad, grad_expand, grad_reduce)


def solution(mesh):
    in_specs = (
        P("section", "dev", None),
        P("dev", None),
        P("section", None),
        P("section", None),
        P("section", None, "dev"),
        P("section", "dev"),
        P("section", "dev"),
        P("section", "dev", None),
        P("section", "dev", None),
        P("section", "dev", None),
        P("dev", None),
        P("section", None, None),
        P("section", None, None),
    )
    out_specs = (
        P("section", "dev", None),
        P("section", "dev", None),
        P("section", None, None),
        P("section", None, None),
    )
    return jax.shard_map(shards, mesh=mesh, in_specs=in_specs, out_specs=out_specs, check_vma=False)
```

```python
import functools
import math

import jax
import jax.numpy as jnp
from jax import lax
from jax.experimental import pallas as pl
from jax.experimental.pallas import tpu as pltpu
from jax.sharding import PartitionSpec as P

epsilon = 1e-05
bf16 = jnp.bfloat16
f32 = jnp.float32


def from_behind(x, axis, by):
    peers = lax.axis_size(axis)
    pairs = [(i, i + by) for i in range(peers) if 0 <= i + by < peers]
    return lax.ppermute(x, axis, pairs)


def swap(x):
    return lax.ppermute(x, "dev", [(i, i ^ 1) for i in range(lax.axis_size("dev"))])


def partner(chip, step, count):
    return chip ^ step if count & (count - 1) == 0 else lax.rem(chip + step, count)


def across(x, step, back=False):
    count = lax.axis_size("dev") // 2
    pairs = []
    for chip in range(count):
        other = chip ^ step if count & (count - 1) == 0 else (chip + step) % count
        for core in range(2):
            here, there = 2 * chip + core, 2 * other + core
            pairs.append((there, here) if back else (here, there))
    return lax.ppermute(x, "dev", pairs)


def in_pairs(count):
    return count >= 4 and count & (count - 1) == 0


def gather(x):
    count = lax.axis_size("dev") // 2
    got = {0: x}
    if not in_pairs(count):
        for step in range(count - 1, 0, -1):
            got[step] = across(x, step, back=True)
        return got
    far = range(count - 2, 0, -2)
    for step in far:
        got[step] = across(x, step)
    got[1] = across(x, 1)
    for step in far:
        got[step ^ 1] = across(got[step], 1)
    return got


def scatter(pieces):
    count = lax.axis_size("dev") // 2
    if not in_pairs(count):
        return [across(pieces[step].astype(bf16), step) for step in range(count - 1, 0, -1)]
    far = range(count - 2, 0, -2)
    inner = {}
    for step in far:
        inner[step] = across(pieces[step ^ 1], 1)
    terms = [across(pieces[1], 1)]
    for step in far:
        both = (pieces[step].astype(f32) + inner[step].astype(f32)).astype(bf16)
        terms.append(across(both, step))
    return terms


def piece_type(step, count):
    return f32 if in_pairs(count) and step % 2 == 0 else bf16


def whole_arrays(body, outs, args, flops=0, scratch=(), mib=24):
    moved = sum(math.prod(a.shape) * a.dtype.itemsize for a in (*args, *outs))
    return pl.pallas_call(
        body,
        out_shape=list(outs),
        in_specs=[pl.BlockSpec(memory_space=pltpu.VMEM)] * len(args),
        out_specs=[pl.BlockSpec(memory_space=pltpu.VMEM)] * len(outs),
        scratch_shapes=list(scratch),
        compiler_params=pltpu.CompilerParams(vmem_limit_bytes=mib * 2**20),
        cost_estimate=pl.CostEstimate(
            flops=max(flops, moved), bytes_accessed=moved, transcendentals=0
        ),
    )(*args)


def shape(dims, dtype):
    return jax.ShapeDtypeStruct(dims, dtype)


def tile_of(extent, limit, unit):
    fitting = [t for t in range(unit, limit + 1, unit) if extent % t == 0]
    return fitting[-1] if fitting else extent


def tiles(extent, tile):
    def each(body):
        @pl.loop(0, extent // tile)
        def _(index):
            body(pl.ds(pl.multiple_of(index * tile, tile), tile))

    return each


def affine(sums, squares, count, gain, shift):
    average = sums / count
    second = squares / count
    spread = gain * lax.rsqrt(second - average * average + epsilon)
    return (spread, shift - average * spread)


def silu(values):
    return values * jax.nn.sigmoid(values)


def early_pre_kernel(saved, weight, act, bend):
    @tiles(saved.shape[0], tile_of(saved.shape[0], 256, 16))
    def _(rows):
        pre = jnp.dot(saved[rows, :], weight[...], preferred_element_type=f32)
        sigma = jax.nn.sigmoid(pre)
        act[rows, :] = (pre * sigma).astype(bf16)
        bend[rows, :] = (sigma * (1.0 + pre * (1.0 - sigma))).astype(bf16)


def early_grads_kernel(sections, saved, leaving, arrived, act, bend, weight, grad, slope, keep, send):
    last = lax.axis_index("section") == sections - 1
    first_core = lax.rem(lax.axis_index("dev"), 2) == 0

    @tiles(saved.shape[0], tile_of(saved.shape[0], 256, 16))
    def _(rows):
        here = jnp.where(last, leaving[rows, :], arrived[rows, :])
        grad[rows, :] = here
        back = lax.dot_general(
            here, weight[...], (((1,), (1,)), ((), ())), preferred_element_type=f32
        )
        slope[rows, :] = (back * bend[rows, :].astype(f32)).astype(bf16)

    over_rows = (((0,), (0,)), ((), ()))
    one = lax.dot_general(saved[...], slope[...], over_rows, preferred_element_type=f32)
    two = lax.dot_general(grad[...], act[...], over_rows, preferred_element_type=f32)
    keep[...] = jnp.where(first_core, one, two)
    send[...] = jnp.where(first_core, two, one).astype(bf16)


def pieces_kernel(count, keep, got, own, *pieces):
    chip = lax.div(lax.axis_index("dev"), 2)
    extent = own.shape[0]

    def piece(index):
        rows = pl.ds(pl.multiple_of(index * extent, extent), extent)
        return keep[rows, :] + got[rows, :].astype(f32)

    own[...] = piece(chip)
    for step in range(1, count):
        out = pieces[step - 1]
        out[...] = piece(partner(chip, step, count)).astype(out.dtype)


def total_kernel(factor, own, *refs):
    total = own[...]
    for got in refs[:-1]:
        total = total + got[...].astype(f32)
    refs[-1][...] = (total * factor).astype(bf16)


def assemble_kernel(count, *refs):
    mine, theirs = refs[:count], refs[count : 2 * count]
    expand, reduce, held = refs[2 * count :]
    chip = lax.div(lax.axis_index("dev"), 2)
    first_core = lax.rem(lax.axis_index("dev"), 2) == 0
    extent = mine[0].shape[0]
    for step in range(count):
        index = partner(chip, step, count) if step else chip
        rows = pl.ds(pl.multiple_of(index * extent, extent), extent)
        one, two = mine[step][...].astype(f32), theirs[step][...].astype(f32)
        expand[rows, :] = jnp.where(first_core, one, two)
        held[rows, :] = jnp.where(first_core, two, one)

    @tiles(held.shape[1], tile_of(held.shape[1], 256, 128))
    def _(columns):
        reduce[columns, :] = held[:, columns].T


def late_sums_kernel(*refs):
    sums = 0.0
    squares = 0.0
    for block in refs[:-1]:
        values = block[...].astype(f32)
        sums = sums + jnp.sum(values, axis=0, keepdims=True)
        squares = squares + jnp.sum(values * values, axis=0, keepdims=True)
    refs[-1][...] = jnp.concatenate([sums, squares], axis=0)


def late_inner_kernel(count, total_rows, *refs):
    blocks = refs[:count]
    mine, got, gain, shift, weight, weight_two, inner, sums, swapped, first = refs[count:]
    spread, offset = affine(
        mine[0:1, :] + got[0:1, :], mine[1:2, :] + got[1:2, :], total_rows, gain[...], shift[...]
    )
    used, held = blocks[0].shape[0], first.shape[0] // count
    if used < held:
        first[...] = jnp.zeros_like(first)
    for index, block in enumerate(blocks):
        values = silu(block[...].astype(f32) * spread + offset).astype(bf16)
        first[index * held : index * held + used, :] = values
    hidden = weight.shape[1]
    tile = tile_of(hidden, 256, 128)
    for part, source in enumerate((weight, weight_two)):
        for start in range(0, hidden, tile):
            term = jnp.dot(first[...], source[:, start : start + tile], preferred_element_type=f32)
            here = slice(part * hidden + start, part * hidden + start + tile)
            there = slice((1 - part) * hidden + start, (1 - part) * hidden + start + tile)
            inner[:, here] = term
            both = jnp.concatenate(
                [
                    jnp.sum(term, axis=0, keepdims=True),
                    jnp.sum(term * term, axis=0, keepdims=True),
                ],
                axis=0,
            )
            sums[:, here] = both
            swapped[:, there] = both


def late_hidden_kernel(
    count, total_rows, inner, sums, got, one, two, weight, weight_two, rows, own, *refs
):
    partials, hidden = refs[:-1], refs[-1]
    extent = weight.shape[0]
    for part, gain_shift in enumerate((one, two)):
        here = slice(part * extent, (part + 1) * extent)
        spread, offset = affine(
            sums[0:1, here] + got[0:1, here],
            sums[1:2, here] + got[1:2, here],
            total_rows,
            gain_shift[0:1, :],
            gain_shift[1:2, :],
        )
        hidden[:, here] = silu(inner[:, here] * spread + offset).astype(bf16)
    used, held = rows.shape[0], inner.shape[0] // count
    tile = tile_of(weight.shape[1], 256, 128)
    for start in range(0, weight.shape[1], tile):
        columns = slice(start, start + tile)
        term = jnp.dot(hidden[:, :extent], weight[:, columns], preferred_element_type=f32)
        term = term + jnp.dot(
            hidden[:, extent:], weight_two[:, columns], preferred_element_type=f32
        )
        own[:, columns] = rows[:, columns].astype(f32) + term[:used]
        for step in range(1, count):
            out = partials[step - 1]
            out[:, columns] = term[step * held : step * held + used].astype(out.dtype)


def late_total_kernel(own, *refs):
    total = own[...]
    for got in refs[:-1]:
        total = total + got[...].astype(f32)
    refs[-1][...] = total.astype(bf16)


def shards(
    late_sent,
    entry_rows,
    gain_first,
    shift_first,
    expand_late,
    gain_inner,
    shift_inner,
    reduce_late,
    early_saved,
    upstream_grad,
    exit_grad,
    expand_early,
    reduce_early,
):
    sections, count = lax.axis_size("section"), lax.axis_size("dev") // 2
    section = lax.axis_index("section")
    steps = range(1, count)

    late_arrived = from_behind(late_sent[0], "section", 1)
    early_arrived = from_behind(upstream_grad[0], "section", -1)
    expand_two, reduce_two = swap(expand_late[0]), swap(reduce_late[0])
    one = jnp.concatenate([gain_inner, shift_inner], axis=0)
    two = swap(one)

    own_rows = jnp.where(section == 0, entry_rows, late_arrived)
    blocks = gather(own_rows)

    saved = early_saved[0]
    pixels, narrow = saved.shape
    wide = expand_early.shape[2]
    work = 2 * pixels * narrow * wide
    act, bend = whole_arrays(
        early_pre_kernel, [shape((pixels, wide), bf16)] * 2, [saved, expand_early[0]], work
    )
    grad, slope, keep, send = whole_arrays(
        functools.partial(early_grads_kernel, sections),
        [
            shape((pixels, narrow), bf16),
            shape((pixels, wide), bf16),
            shape((narrow, wide), f32),
            shape((narrow, wide), bf16),
        ],
        [saved, exit_grad, early_arrived, act, bend, reduce_early[0]],
        3 * work,
    )
    got = swap(send)
    share = narrow // count
    own_share, *shares = whole_arrays(
        functools.partial(pieces_kernel, count),
        [shape((share, wide), f32)]
        + [shape((share, wide), piece_type(step, count)) for step in steps],
        [keep, got],
    )
    terms = scatter(dict(zip(steps, shares)))

    rows, channels = own_rows.shape
    total_rows = rows * lax.axis_size("dev")
    held = -(-rows // 16) * 16
    hidden = expand_late.shape[2]
    late_work = 4 * count * held * channels * hidden
    listed = lax.optimization_barrier(tuple(blocks[step] for step in range(count)) + (own_share,))
    listed, own_share = list(listed[:-1]), listed[-1]
    (mine,) = whole_arrays(late_sums_kernel, [shape((2, channels), f32)], listed)
    others = swap(mine)
    inner, sums, swapped = whole_arrays(
        functools.partial(late_inner_kernel, count, total_rows),
        [shape((count * held, 2 * hidden), f32), shape((2, 2 * hidden), f32), shape((2, 2 * hidden), f32)],
        listed + [mine, others, gain_first, shift_first, expand_late[0], expand_two],
        late_work,
        [pltpu.VMEM((count * held, channels), bf16)],
    )
    got_sums = swap(swapped)
    own_late, *partials = whole_arrays(
        functools.partial(late_hidden_kernel, count, total_rows),
        [shape((rows, channels), f32)]
        + [shape((rows, channels), piece_type(step, count)) for step in steps],
        [inner, sums, got_sums, one, two, reduce_late[0], reduce_two, own_rows],
        late_work,
        [pltpu.VMEM((count * held, 2 * hidden), bf16)],
    )
    late_terms = scatter(dict(zip(steps, partials)))

    factor = 1.0 / math.sqrt(pixels * lax.axis_size("dev"))
    (summed,) = whole_arrays(
        functools.partial(total_kernel, factor), [shape((share, wide), bf16)], [own_share] + terms
    )
    gathered = gather(summed)
    theirs = {step: swap(gathered[step]) for step in gathered}
    input_grad = grad.astype(f32) + lax.dot_general(
        slope, expand_early[0], (((1,), (1,)), ((), ())), preferred_element_type=f32
    )
    input_grad = input_grad.astype(bf16)
    grad_expand, grad_reduce = whole_arrays(
        functools.partial(assemble_kernel, count),
        [shape((narrow, wide), f32), shape((wide, narrow), f32)],
        [gathered[step] for step in range(count)] + [theirs[step] for step in range(count)],
        scratch=[pltpu.VMEM((narrow, wide), f32)],
    )
    (late_out,) = whole_arrays(
        late_total_kernel, [shape((rows, channels), bf16)], [own_late] + late_terms
    )
    return (late_out[None], input_grad[None], grad_expand[None], grad_reduce[None])


def solution(mesh):
    in_specs = (
        P("section", "dev", None),
        P("dev", None),
        P("section", None),
        P("section", None),
        P("section", None, "dev"),
        P("section", "dev"),
        P("section", "dev"),
        P("section", "dev", None),
        P("section", "dev", None),
        P("section", "dev", None),
        P("dev", None),
        P("section", None, None),
        P("section", None, None),
    )
    out_specs = (
        P("section", "dev", None),
        P("section", "dev", None),
        P("section", None, None),
        P("section", None, None),
    )
    return jax.shard_map(shards, mesh=mesh, in_specs=in_specs, out_specs=out_specs, check_vma=False)
```

```python
import functools
import math

import jax
import jax.numpy as jnp
from jax import lax
from jax.experimental import pallas as pl
from jax.experimental.pallas import tpu as pltpu
from jax.sharding import PartitionSpec as P

epsilon = 1e-05
bf16 = jnp.bfloat16
f32 = jnp.float32


def from_behind(x, axis, by):
    peers = lax.axis_size(axis)
    pairs = [(i, i + by) for i in range(peers) if 0 <= i + by < peers]
    return lax.ppermute(x, axis, pairs)


def swap(x):
    return lax.ppermute(x, "dev", [(i, i ^ 1) for i in range(lax.axis_size("dev"))])


def partner(chip, step, count):
    return chip ^ step if count & (count - 1) == 0 else lax.rem(chip + step, count)


def across(x, step, back=False):
    count = lax.axis_size("dev") // 2
    pairs = []
    for chip in range(count):
        other = chip ^ step if count & (count - 1) == 0 else (chip + step) % count
        for core in range(2):
            here, there = 2 * chip + core, 2 * other + core
            pairs.append((there, here) if back else (here, there))
    return lax.ppermute(x, "dev", pairs)


def in_pairs(count):
    return count >= 4 and count & (count - 1) == 0


def gather(x):
    count = lax.axis_size("dev") // 2
    got = {0: x}
    if not in_pairs(count):
        for step in range(count - 1, 0, -1):
            got[step] = across(x, step, back=True)
        return got
    far = range(count - 2, 0, -2)
    for step in far:
        got[step] = across(x, step)
    got[1] = across(x, 1)
    for step in far:
        got[step ^ 1] = across(got[step], 1)
    return got


def scatter(pieces):
    count = lax.axis_size("dev") // 2
    if not in_pairs(count):
        return [across(pieces[step].astype(bf16), step) for step in range(count - 1, 0, -1)]
    far = range(count - 2, 0, -2)
    inner = {}
    for step in far:
        inner[step] = across(pieces[step ^ 1], 1)
    terms = [across(pieces[1], 1)]
    for step in far:
        both = (pieces[step].astype(f32) + inner[step].astype(f32)).astype(bf16)
        terms.append(across(both, step))
    return terms


def piece_type(step, count):
    return f32 if in_pairs(count) and step % 2 == 0 else bf16


def whole_arrays(body, outs, args, flops=0, scratch=(), mib=24):
    moved = sum(math.prod(a.shape) * a.dtype.itemsize for a in (*args, *outs))
    return pl.pallas_call(
        body,
        out_shape=list(outs),
        in_specs=[pl.BlockSpec(memory_space=pltpu.VMEM)] * len(args),
        out_specs=[pl.BlockSpec(memory_space=pltpu.VMEM)] * len(outs),
        scratch_shapes=list(scratch),
        compiler_params=pltpu.CompilerParams(vmem_limit_bytes=mib * 2**20),
        cost_estimate=pl.CostEstimate(
            flops=max(flops, moved), bytes_accessed=moved, transcendentals=0
        ),
    )(*args)


def shape(dims, dtype):
    return jax.ShapeDtypeStruct(dims, dtype)


def tile_of(extent, limit, unit):
    fitting = [t for t in range(unit, limit + 1, unit) if extent % t == 0]
    return fitting[-1] if fitting else extent


def tiles(extent, tile):
    def each(body):
        @pl.loop(0, extent // tile)
        def _(index):
            body(pl.ds(pl.multiple_of(index * tile, tile), tile))

    return each


def affine(sums, squares, count, gain, shift):
    average = sums / count
    second = squares / count
    spread = gain * lax.rsqrt(second - average * average + epsilon)
    return (spread, shift - average * spread)


def silu(values):
    return values * jax.nn.sigmoid(values)


def cut_kernel(starts, whole, *refs):
    for part, ref in enumerate(refs):
        ref[...] = whole[starts[part] : starts[part + 1], :]


def early_pre_kernel(starts, saved, weight, *refs):
    parts = len(starts) - 1
    for part in range(parts):
        act, bend = refs[2 * part : 2 * part + 2]
        first, extent = starts[part], starts[part + 1] - starts[part]
        tile = tile_of(extent, 256, 16)

        @pl.loop(0, extent // tile)
        def _(index):
            here = pl.ds(pl.multiple_of(index * tile, tile), tile)
            rows = pl.ds(pl.multiple_of(first + index * tile, 16), tile)
            pre = jnp.dot(saved[rows, :], weight[...], preferred_element_type=f32)
            sigma = jax.nn.sigmoid(pre)
            act[here, :] = (pre * sigma).astype(bf16)
            bend[here, :] = (sigma * (1.0 + pre * (1.0 - sigma))).astype(bf16)

        if part:
            refs[2 * parts + part - 1][...] = saved[first : first + extent, :]


def early_grads_kernel(sections, first, last_part, saved, leaving, arrived, act, bend, weight, *refs):
    last = lax.axis_index("section") == sections - 1
    extent = arrived.shape[0]
    before, (grad, slope, one_out, two_out) = refs[:-4], refs[-4:]
    tile = tile_of(extent, 672, 16)

    @pl.loop(0, extent // tile)
    def _(index):
        rows = pl.ds(pl.multiple_of(index * tile, tile), tile)
        whole = pl.ds(pl.multiple_of(first + index * tile, 16), tile)
        here = jnp.where(last, leaving[whole, :], arrived[rows, :])
        grad[rows, :] = here
        back = lax.dot_general(
            here, weight[...], (((1,), (1,)), ((), ())), preferred_element_type=f32
        )
        slope[rows, :] = (back * bend[rows, :].astype(f32)).astype(bf16)

    over_rows = (((0,), (0,)), ((), ()))
    one = lax.dot_general(saved[:extent, :], slope[...], over_rows, preferred_element_type=f32)
    two = lax.dot_general(grad[...], act[...], over_rows, preferred_element_type=f32)
    if before:
        one, two = one + before[0][...], two + before[1][...]
    if last_part:
        first_core = lax.rem(lax.axis_index("dev"), 2) == 0
        one_out[...] = jnp.where(first_core, one, two)
        two_out[...] = jnp.where(first_core, two, one).astype(bf16)
    else:
        one_out[...] = one
        two_out[...] = two


def input_grad_kernel(parts, weight, *refs):
    out, start = refs[-1], 0
    for part in range(parts):
        grad, slope = refs[2 * part : 2 * part + 2]
        extent = grad.shape[0]
        tile = tile_of(extent, 1024, 16)
        first = start

        @pl.loop(0, extent // tile)
        def _(index):
            rows = pl.ds(pl.multiple_of(index * tile, tile), tile)
            whole = pl.ds(pl.multiple_of(first + index * tile, 16), tile)
            term = lax.dot_general(
                slope[rows, :], weight[...], (((1,), (1,)), ((), ())), preferred_element_type=f32
            )
            out[whole, :] = (grad[rows, :].astype(f32) + term).astype(bf16)

        start += extent


def pieces_kernel(count, keep, got, own, *pieces):
    chip = lax.div(lax.axis_index("dev"), 2)
    extent = own.shape[0]

    def piece(index):
        rows = pl.ds(pl.multiple_of(index * extent, extent), extent)
        return keep[rows, :] + got[rows, :].astype(f32)

    own[...] = piece(chip)
    for step in range(1, count):
        out = pieces[step - 1]
        out[...] = piece(partner(chip, step, count)).astype(out.dtype)


def total_kernel(factor, own, *refs):
    total = own[...]
    for got in refs[:-1]:
        total = total + got[...].astype(f32)
    refs[-1][...] = (total * factor).astype(bf16)


def assemble_kernel(count, *refs):
    mine, theirs = refs[:count], refs[count : 2 * count]
    expand, reduce, held = refs[2 * count :]
    chip = lax.div(lax.axis_index("dev"), 2)
    first_core = lax.rem(lax.axis_index("dev"), 2) == 0
    extent = mine[0].shape[0]
    for step in range(count):
        index = partner(chip, step, count) if step else chip
        rows = pl.ds(pl.multiple_of(index * extent, extent), extent)
        one, two = mine[step][...].astype(f32), theirs[step][...].astype(f32)
        expand[rows, :] = jnp.where(first_core, one, two)
        held[rows, :] = jnp.where(first_core, two, one)

    @tiles(held.shape[1], tile_of(held.shape[1], 256, 128))
    def _(columns):
        reduce[columns, :] = held[:, columns].T


def late_sums_kernel(*refs):
    sums = 0.0
    squares = 0.0
    for block in refs[:-1]:
        values = block[...].astype(f32)
        sums = sums + jnp.sum(values, axis=0, keepdims=True)
        squares = squares + jnp.sum(values * values, axis=0, keepdims=True)
    refs[-1][...] = jnp.concatenate([sums, squares], axis=0)


def late_inner_kernel(count, total_rows, *refs):
    blocks = refs[:count]
    mine, got, gain, shift, weight, weight_two, inner, sums, swapped, first = refs[count:]
    spread, offset = affine(
        mine[0:1, :] + got[0:1, :], mine[1:2, :] + got[1:2, :], total_rows, gain[...], shift[...]
    )
    used, held = blocks[0].shape[0], first.shape[0] // count
    if used < held:
        first[...] = jnp.zeros_like(first)
    for index, block in enumerate(blocks):
        values = silu(block[...].astype(f32) * spread + offset).astype(bf16)
        first[index * held : index * held + used, :] = values
    hidden = weight.shape[1]
    tile = tile_of(hidden, 256, 128)
    for part, source in enumerate((weight, weight_two)):
        for start in range(0, hidden, tile):
            term = jnp.dot(first[...], source[:, start : start + tile], preferred_element_type=f32)
            here = slice(part * hidden + start, part * hidden + start + tile)
            there = slice((1 - part) * hidden + start, (1 - part) * hidden + start + tile)
            inner[:, here] = term
            both = jnp.concatenate(
                [
                    jnp.sum(term, axis=0, keepdims=True),
                    jnp.sum(term * term, axis=0, keepdims=True),
                ],
                axis=0,
            )
            sums[:, here] = both
            swapped[:, there] = both


def late_hidden_kernel(
    count, total_rows, inner, sums, got, one, two, weight, weight_two, rows, own, *refs
):
    partials, hidden = refs[:-1], refs[-1]
    extent = weight.shape[0]
    for part, gain_shift in enumerate((one, two)):
        here = slice(part * extent, (part + 1) * extent)
        spread, offset = affine(
            sums[0:1, here] + got[0:1, here],
            sums[1:2, here] + got[1:2, here],
            total_rows,
            gain_shift[0:1, :],
            gain_shift[1:2, :],
        )
        hidden[:, here] = silu(inner[:, here] * spread + offset).astype(bf16)
    used, held = rows.shape[0], inner.shape[0] // count
    tile = tile_of(weight.shape[1], 256, 128)
    for start in range(0, weight.shape[1], tile):
        columns = slice(start, start + tile)
        term = jnp.dot(hidden[:, :extent], weight[:, columns], preferred_element_type=f32)
        term = term + jnp.dot(
            hidden[:, extent:], weight_two[:, columns], preferred_element_type=f32
        )
        own[:, columns] = rows[:, columns].astype(f32) + term[:used]
        for step in range(1, count):
            out = partials[step - 1]
            out[:, columns] = term[step * held : step * held + used].astype(out.dtype)


def late_total_kernel(own, *refs):
    total = own[...]
    for got in refs[:-1]:
        total = total + got[...].astype(f32)
    refs[-1][...] = total.astype(bf16)


def shards(
    late_sent,
    entry_rows,
    gain_first,
    shift_first,
    expand_late,
    gain_inner,
    shift_inner,
    reduce_late,
    early_saved,
    upstream_grad,
    exit_grad,
    expand_early,
    reduce_early,
):
    sections, count = lax.axis_size("section"), lax.axis_size("dev") // 2
    section = lax.axis_index("section")
    steps = range(1, count)

    late_arrived = from_behind(late_sent[0], "section", 1)
    pixels = upstream_grad.shape[1]
    tail = 2 * tile_of(pixels, 256, 16)
    starts = (0, pixels - tail, pixels) if tail < pixels else (0, pixels)
    parts = len(starts) - 1
    extents = [starts[part + 1] - starts[part] for part in range(parts)]
    leaving = whole_arrays(
        functools.partial(cut_kernel, starts),
        [shape((extent, upstream_grad.shape[2]), bf16) for extent in extents],
        [upstream_grad[0]],
    )
    early_arrived = []
    for part in range(parts):
        early_arrived.append(from_behind(leaving[part], "section", -1))
    expand_two, reduce_two = swap(expand_late[0]), swap(reduce_late[0])
    one = jnp.concatenate([gain_inner, shift_inner], axis=0)
    two = swap(one)

    own_rows = jnp.where(section == 0, entry_rows, late_arrived)
    blocks = gather(own_rows)

    saved = early_saved[0]
    narrow, wide = expand_early.shape[1:]
    work = 2 * narrow * wide
    pre = whole_arrays(
        functools.partial(early_pre_kernel, starts),
        [shape((extents[part // 2], wide), bf16) for part in range(2 * parts)]
        + [shape((extent, narrow), bf16) for extent in extents[1:]],
        [saved, expand_early[0]],
        pixels * work,
    )
    grads, sums_so_far = [], []
    for part in range(parts):
        final = part == parts - 1
        grad, slope, keep, send = whole_arrays(
            functools.partial(early_grads_kernel, sections, starts[part], final),
            [
                shape((extents[part], narrow), bf16),
                shape((extents[part], wide), bf16),
                shape((narrow, wide), f32),
                shape((narrow, wide), bf16 if final else f32),
            ],
            [
                pre[2 * parts + part - 1] if part else saved,
                exit_grad,
                early_arrived[part],
                *pre[2 * part : 2 * part + 2],
                reduce_early[0],
                *sums_so_far,
            ],
            3 * extents[part] * work,
        )
        grads += [grad, slope]
        sums_so_far = [keep, send]
    got = swap(send)
    share = narrow // count
    own_share, *shares = whole_arrays(
        functools.partial(pieces_kernel, count),
        [shape((share, wide), f32)]
        + [shape((share, wide), piece_type(step, count)) for step in steps],
        [keep, got],
    )
    terms = scatter(dict(zip(steps, shares)))

    rows, channels = own_rows.shape
    total_rows = rows * lax.axis_size("dev")
    held = -(-rows // 16) * 16
    hidden = expand_late.shape[2]
    late_work = 4 * count * held * channels * hidden
    listed = [blocks[step] for step in range(count)]
    (mine,) = whole_arrays(late_sums_kernel, [shape((2, channels), f32)], listed)
    others = swap(mine)
    inner, sums, swapped = whole_arrays(
        functools.partial(late_inner_kernel, count, total_rows),
        [shape((count * held, 2 * hidden), f32), shape((2, 2 * hidden), f32), shape((2, 2 * hidden), f32)],
        listed + [mine, others, gain_first, shift_first, expand_late[0], expand_two],
        late_work,
        [pltpu.VMEM((count * held, channels), bf16)],
    )
    got_sums = swap(swapped)
    own_late, *partials = whole_arrays(
        functools.partial(late_hidden_kernel, count, total_rows),
        [shape((rows, channels), f32)]
        + [shape((rows, channels), piece_type(step, count)) for step in steps],
        [inner, sums, got_sums, one, two, reduce_late[0], reduce_two, own_rows],
        late_work,
        [pltpu.VMEM((count * held, 2 * hidden), bf16)],
    )
    late_terms = scatter(dict(zip(steps, partials)))

    factor = 1.0 / math.sqrt(pixels * lax.axis_size("dev"))
    (summed,) = whole_arrays(
        functools.partial(total_kernel, factor), [shape((share, wide), bf16)], [own_share] + terms
    )
    gathered = gather(summed)
    theirs = {step: swap(gathered[step]) for step in gathered}
    (input_grad,) = whole_arrays(
        functools.partial(input_grad_kernel, parts),
        [shape((pixels, narrow), bf16)],
        [expand_early[0], *grads],
        pixels * work,
    )
    grad_expand, grad_reduce = whole_arrays(
        functools.partial(assemble_kernel, count),
        [shape((narrow, wide), f32), shape((wide, narrow), f32)],
        [gathered[step] for step in range(count)] + [theirs[step] for step in range(count)],
        scratch=[pltpu.VMEM((narrow, wide), f32)],
    )
    (late_out,) = whole_arrays(
        late_total_kernel, [shape((rows, channels), bf16)], [own_late] + late_terms
    )
    return (late_out[None], input_grad[None], grad_expand[None], grad_reduce[None])


def solution(mesh):
    in_specs = (
        P("section", "dev", None),
        P("dev", None),
        P("section", None),
        P("section", None),
        P("section", None, "dev"),
        P("section", "dev"),
        P("section", "dev"),
        P("section", "dev", None),
        P("section", "dev", None),
        P("section", "dev", None),
        P("dev", None),
        P("section", None, None),
        P("section", None, None),
    )
    out_specs = (
        P("section", "dev", None),
        P("section", "dev", None),
        P("section", None, None),
        P("section", None, None),
    )
    return jax.shard_map(shards, mesh=mesh, in_specs=in_specs, out_specs=out_specs, check_vma=False)
```

```python
import functools
import math

import jax
import jax.numpy as jnp
from jax import lax
from jax.experimental import pallas as pl
from jax.experimental.pallas import tpu as pltpu
from jax.sharding import PartitionSpec as P

epsilon = 1e-05
bf16 = jnp.bfloat16
f32 = jnp.float32


def from_behind(x, axis, by):
    peers = lax.axis_size(axis)
    pairs = [(i, i + by) for i in range(peers) if 0 <= i + by < peers]
    return lax.ppermute(x, axis, pairs)


def swap(x):
    return lax.ppermute(x, "dev", [(i, i ^ 1) for i in range(lax.axis_size("dev"))])


def partner(chip, step, count):
    return chip ^ step if count & (count - 1) == 0 else lax.rem(chip + step, count)


def across(x, step, back=False):
    count = lax.axis_size("dev") // 2
    pairs = []
    for chip in range(count):
        other = chip ^ step if count & (count - 1) == 0 else (chip + step) % count
        for core in range(2):
            here, there = 2 * chip + core, 2 * other + core
            pairs.append((there, here) if back else (here, there))
    return lax.ppermute(x, "dev", pairs)


def in_pairs(count):
    return count >= 4 and count & (count - 1) == 0


def gather(x):
    count = lax.axis_size("dev") // 2
    got = {0: x}
    if not in_pairs(count):
        for step in range(count - 1, 0, -1):
            got[step] = across(x, step, back=True)
        return got
    far = range(count - 2, 0, -2)
    for step in far:
        got[step] = across(x, step)
    got[1] = across(x, 1)
    for step in far:
        got[step ^ 1] = across(got[step], 1)
    return got


def scatter(pieces):
    count = lax.axis_size("dev") // 2
    if not in_pairs(count):
        return [across(pieces[step].astype(bf16), step) for step in range(count - 1, 0, -1)]
    far = range(count - 2, 0, -2)
    inner = {}
    for step in far:
        inner[step] = across(pieces[step ^ 1], 1)
    terms = [across(pieces[1], 1)]
    for step in far:
        both = (pieces[step].astype(f32) + inner[step].astype(f32)).astype(bf16)
        terms.append(across(both, step))
    return terms


def inner_steps(count):
    return list(range(count - 1, 2, -2)) if in_pairs(count) else []


def piece_type(step, count):
    return f32 if in_pairs(count) and step % 2 == 0 else bf16


def whole_arrays(body, outs, args, flops=0, scratch=(), mib=24):
    moved = sum(math.prod(a.shape) * a.dtype.itemsize for a in (*args, *outs))
    return pl.pallas_call(
        body,
        out_shape=list(outs),
        in_specs=[pl.BlockSpec(memory_space=pltpu.VMEM)] * len(args),
        out_specs=[pl.BlockSpec(memory_space=pltpu.VMEM)] * len(outs),
        scratch_shapes=list(scratch),
        compiler_params=pltpu.CompilerParams(vmem_limit_bytes=mib * 2**20),
        cost_estimate=pl.CostEstimate(
            flops=max(flops, moved), bytes_accessed=moved, transcendentals=0
        ),
    )(*args)


def shape(dims, dtype):
    return jax.ShapeDtypeStruct(dims, dtype)


def tile_of(extent, limit, unit):
    fitting = [t for t in range(unit, limit + 1, unit) if extent % t == 0]
    return fitting[-1] if fitting else extent


def tiles(extent, tile):
    def each(body):
        @pl.loop(0, extent // tile)
        def _(index):
            body(pl.ds(pl.multiple_of(index * tile, tile), tile))

    return each


def affine(sums, squares, count, gain, shift):
    average = sums / count
    second = squares / count
    spread = gain * lax.rsqrt(second - average * average + epsilon)
    return (spread, shift - average * spread)


def silu(values):
    return values * jax.nn.sigmoid(values)


def cut_kernel(starts, whole, *refs):
    for part, ref in enumerate(refs):
        ref[...] = whole[starts[part] : starts[part + 1], :]


def early_pre_kernel(starts, saved, weight, *refs):
    parts = len(starts) - 1
    for part in range(parts):
        act, bend = refs[2 * part : 2 * part + 2]
        first, extent = starts[part], starts[part + 1] - starts[part]
        tile = tile_of(extent, 256, 16)

        @pl.loop(0, extent // tile)
        def _(index):
            here = pl.ds(pl.multiple_of(index * tile, tile), tile)
            rows = pl.ds(pl.multiple_of(first + index * tile, 16), tile)
            pre = jnp.dot(saved[rows, :], weight[...], preferred_element_type=f32)
            sigma = jax.nn.sigmoid(pre)
            act[here, :] = (pre * sigma).astype(bf16)
            bend[here, :] = (sigma * (1.0 + pre * (1.0 - sigma))).astype(bf16)

        if part:
            refs[2 * parts + part - 1][...] = saved[first : first + extent, :]


def early_grads_kernel(sections, count, first, last_part, saved, leaving, arrived, act, bend, weight, *refs):
    last = lax.axis_index("section") == sections - 1
    extent = arrived.shape[0]
    outs = 4 + len(inner_steps(count)) if last_part else 4
    before, (grad, slope, one_out, two_out, *urgent) = refs[:-outs], refs[-outs:]
    tile = tile_of(extent, 672, 16)

    @pl.loop(0, extent // tile)
    def _(index):
        rows = pl.ds(pl.multiple_of(index * tile, tile), tile)
        whole = pl.ds(pl.multiple_of(first + index * tile, 16), tile)
        here = jnp.where(last, leaving[whole, :], arrived[rows, :])
        grad[rows, :] = here
        back = lax.dot_general(
            here, weight[...], (((1,), (1,)), ((), ())), preferred_element_type=f32
        )
        slope[rows, :] = (back * bend[rows, :].astype(f32)).astype(bf16)

    over_rows = (((0,), (0,)), ((), ()))
    one = lax.dot_general(saved[:extent, :], slope[...], over_rows, preferred_element_type=f32)
    two = lax.dot_general(grad[...], act[...], over_rows, preferred_element_type=f32)
    if before:
        one, two = one + before[0][...], two + before[1][...]
    if last_part:
        first_core = lax.rem(lax.axis_index("dev"), 2) == 0
        one_out[...] = jnp.where(first_core, one, two)
        two_out[...] = jnp.where(first_core, two, one).astype(bf16)
        for step, out in zip(inner_steps(count), urgent):
            out[...] = two_out[rows_of(step, count, out.shape[0]), :]
    else:
        one_out[...] = one
        two_out[...] = two


def input_grad_kernel(parts, weight, *refs):
    out, start = refs[-1], 0
    for part in range(parts):
        grad, slope = refs[2 * part : 2 * part + 2]
        extent = grad.shape[0]
        tile = tile_of(extent, 1024, 16)
        first = start

        @pl.loop(0, extent // tile)
        def _(index):
            rows = pl.ds(pl.multiple_of(index * tile, tile), tile)
            whole = pl.ds(pl.multiple_of(first + index * tile, 16), tile)
            term = lax.dot_general(
                slope[rows, :], weight[...], (((1,), (1,)), ((), ())), preferred_element_type=f32
            )
            out[whole, :] = (grad[rows, :].astype(f32) + term).astype(bf16)

        start += extent


def rows_of(step, count, extent):
    chip = lax.div(lax.axis_index("dev"), 2)
    index = partner(chip, step, count) if step else chip
    return pl.ds(pl.multiple_of(index * extent, extent), extent)


def urgent_kernel(count, keep, *refs):
    steps = inner_steps(count)
    for step, got, out in zip(steps, refs[: len(steps)], refs[len(steps) :]):
        rows = rows_of(step, count, out.shape[0])
        out[...] = (keep[rows, :] + got[...].astype(f32)).astype(bf16)


def pieces_kernel(count, steps, keep, got, *pieces):
    for step, out in zip(steps, pieces):
        rows = rows_of(step, count, out.shape[0])
        out[...] = (keep[rows, :] + got[rows, :].astype(f32)).astype(out.dtype)


def total_kernel(factor, own, *refs):
    total = own[...]
    for got in refs[:-1]:
        total = total + got[...].astype(f32)
    refs[-1][...] = (total * factor).astype(bf16)


def assemble_kernel(count, *refs):
    mine, theirs = refs[:count], refs[count : 2 * count]
    expand, reduce, held = refs[2 * count :]
    chip = lax.div(lax.axis_index("dev"), 2)
    first_core = lax.rem(lax.axis_index("dev"), 2) == 0
    extent = mine[0].shape[0]
    for step in range(count):
        index = partner(chip, step, count) if step else chip
        rows = pl.ds(pl.multiple_of(index * extent, extent), extent)
        one, two = mine[step][...].astype(f32), theirs[step][...].astype(f32)
        expand[rows, :] = jnp.where(first_core, one, two)
        held[rows, :] = jnp.where(first_core, two, one)

    @tiles(held.shape[1], tile_of(held.shape[1], 256, 128))
    def _(columns):
        reduce[columns, :] = held[:, columns].T


def late_sums_kernel(*refs):
    sums = 0.0
    squares = 0.0
    for block in refs[:-1]:
        values = block[...].astype(f32)
        sums = sums + jnp.sum(values, axis=0, keepdims=True)
        squares = squares + jnp.sum(values * values, axis=0, keepdims=True)
    refs[-1][...] = jnp.concatenate([sums, squares], axis=0)


def late_inner_kernel(count, total_rows, *refs):
    blocks = refs[:count]
    mine, got, gain, shift, weight, weight_two, inner, sums, swapped, first = refs[count:]
    spread, offset = affine(
        mine[0:1, :] + got[0:1, :], mine[1:2, :] + got[1:2, :], total_rows, gain[...], shift[...]
    )
    used, held = blocks[0].shape[0], first.shape[0] // count
    if used < held:
        first[...] = jnp.zeros_like(first)
    for index, block in enumerate(blocks):
        values = silu(block[...].astype(f32) * spread + offset).astype(bf16)
        first[index * held : index * held + used, :] = values
    hidden = weight.shape[1]
    tile = tile_of(hidden, 256, 128)
    for part, source in enumerate((weight, weight_two)):
        for start in range(0, hidden, tile):
            term = jnp.dot(first[...], source[:, start : start + tile], preferred_element_type=f32)
            here = slice(part * hidden + start, part * hidden + start + tile)
            there = slice((1 - part) * hidden + start, (1 - part) * hidden + start + tile)
            inner[:, here] = term
            both = jnp.concatenate(
                [
                    jnp.sum(term, axis=0, keepdims=True),
                    jnp.sum(term * term, axis=0, keepdims=True),
                ],
                axis=0,
            )
            sums[:, here] = both
            swapped[:, there] = both


def late_hidden_kernel(
    count, total_rows, inner, sums, got, one, two, weight, weight_two, rows, own, *refs
):
    partials, hidden = refs[:-1], refs[-1]
    extent = weight.shape[0]
    for part, gain_shift in enumerate((one, two)):
        here = slice(part * extent, (part + 1) * extent)
        spread, offset = affine(
            sums[0:1, here] + got[0:1, here],
            sums[1:2, here] + got[1:2, here],
            total_rows,
            gain_shift[0:1, :],
            gain_shift[1:2, :],
        )
        hidden[:, here] = silu(inner[:, here] * spread + offset).astype(bf16)
    used, held = rows.shape[0], inner.shape[0] // count
    tile = tile_of(weight.shape[1], 256, 128)
    for start in range(0, weight.shape[1], tile):
        columns = slice(start, start + tile)
        term = jnp.dot(hidden[:, :extent], weight[:, columns], preferred_element_type=f32)
        term = term + jnp.dot(
            hidden[:, extent:], weight_two[:, columns], preferred_element_type=f32
        )
        own[:, columns] = rows[:, columns].astype(f32) + term[:used]
        for step in range(1, count):
            out = partials[step - 1]
            out[:, columns] = term[step * held : step * held + used].astype(out.dtype)


def late_total_kernel(own, *refs):
    total = own[...]
    for got in refs[:-1]:
        total = total + got[...].astype(f32)
    refs[-1][...] = total.astype(bf16)


def shards(
    late_sent,
    entry_rows,
    gain_first,
    shift_first,
    expand_late,
    gain_inner,
    shift_inner,
    reduce_late,
    early_saved,
    upstream_grad,
    exit_grad,
    expand_early,
    reduce_early,
):
    sections, count = lax.axis_size("section"), lax.axis_size("dev") // 2
    section = lax.axis_index("section")
    steps = range(1, count)

    late_arrived = from_behind(late_sent[0], "section", 1)
    pixels = upstream_grad.shape[1]
    tail = 2 * tile_of(pixels, 256, 16)
    starts = (0, pixels - tail, pixels) if tail < pixels else (0, pixels)
    parts = len(starts) - 1
    extents = [starts[part + 1] - starts[part] for part in range(parts)]
    leaving = whole_arrays(
        functools.partial(cut_kernel, starts),
        [shape((extent, upstream_grad.shape[2]), bf16) for extent in extents],
        [upstream_grad[0]],
    )
    early_arrived = []
    for part in range(parts):
        early_arrived.append(from_behind(leaving[part], "section", -1))
    expand_two, reduce_two = swap(expand_late[0]), swap(reduce_late[0])
    one = jnp.concatenate([gain_inner, shift_inner], axis=0)
    two = swap(one)

    own_rows = jnp.where(section == 0, entry_rows, late_arrived)
    blocks = gather(own_rows)

    saved = early_saved[0]
    narrow, wide = expand_early.shape[1:]
    work = 2 * narrow * wide
    pre = whole_arrays(
        functools.partial(early_pre_kernel, starts),
        [shape((extents[part // 2], wide), bf16) for part in range(2 * parts)]
        + [shape((extent, narrow), bf16) for extent in extents[1:]],
        [saved, expand_early[0]],
        pixels * work,
    )
    share = narrow // count
    urgent_steps = inner_steps(count)
    grads, sums_so_far = [], []
    for part in range(parts):
        final = part == parts - 1
        grad, slope, keep, send, *urgent = whole_arrays(
            functools.partial(early_grads_kernel, sections, count, starts[part], final),
            [
                shape((extents[part], narrow), bf16),
                shape((extents[part], wide), bf16),
                shape((narrow, wide), f32),
                shape((narrow, wide), bf16 if final else f32),
            ]
            + [shape((share, wide), bf16)] * (len(urgent_steps) if final else 0),
            [
                pre[2 * parts + part - 1] if part else saved,
                exit_grad,
                early_arrived[part],
                *pre[2 * part : 2 * part + 2],
                reduce_early[0],
                *sums_so_far,
            ],
            3 * extents[part] * work,
        )
        grads += [grad, slope]
        sums_so_far = [keep, send]
    shares = {}
    if urgent_steps:
        got_urgent = [swap(piece) for piece in urgent]
        added = whole_arrays(
            functools.partial(urgent_kernel, count),
            [shape((share, wide), bf16)] * len(urgent),
            [keep, *got_urgent],
        )
        shares.update(zip(urgent_steps, added))
    got = swap(send)
    other_steps = [step for step in range(count) if step not in shares]
    added = whole_arrays(
        functools.partial(pieces_kernel, count, other_steps),
        [shape((share, wide), piece_type(step, count) if step else f32) for step in other_steps],
        [keep, got],
    )
    shares.update(zip(other_steps, added))
    own_share = shares[0]
    terms = scatter(shares)

    rows, channels = own_rows.shape
    total_rows = rows * lax.axis_size("dev")
    held = -(-rows // 16) * 16
    hidden = expand_late.shape[2]
    late_work = 4 * count * held * channels * hidden
    listed = [blocks[step] for step in range(count)]
    (mine,) = whole_arrays(late_sums_kernel, [shape((2, channels), f32)], listed)
    others = swap(mine)
    inner, sums, swapped = whole_arrays(
        functools.partial(late_inner_kernel, count, total_rows),
        [shape((count * held, 2 * hidden), f32), shape((2, 2 * hidden), f32), shape((2, 2 * hidden), f32)],
        listed + [mine, others, gain_first, shift_first, expand_late[0], expand_two],
        late_work,
        [pltpu.VMEM((count * held, channels), bf16)],
    )
    got_sums = swap(swapped)
    own_late, *partials = whole_arrays(
        functools.partial(late_hidden_kernel, count, total_rows),
        [shape((rows, channels), f32)]
        + [shape((rows, channels), piece_type(step, count)) for step in steps],
        [inner, sums, got_sums, one, two, reduce_late[0], reduce_two, own_rows],
        late_work,
        [pltpu.VMEM((count * held, 2 * hidden), bf16)],
    )
    late_terms = scatter(dict(zip(steps, partials)))

    factor = 1.0 / math.sqrt(pixels * lax.axis_size("dev"))
    (summed,) = whole_arrays(
        functools.partial(total_kernel, factor), [shape((share, wide), bf16)], [own_share] + terms
    )
    gathered = gather(summed)
    theirs = {step: swap(gathered[step]) for step in gathered}
    (input_grad,) = whole_arrays(
        functools.partial(input_grad_kernel, parts),
        [shape((pixels, narrow), bf16)],
        [expand_early[0], *grads],
        pixels * work,
    )
    grad_expand, grad_reduce = whole_arrays(
        functools.partial(assemble_kernel, count),
        [shape((narrow, wide), f32), shape((wide, narrow), f32)],
        [gathered[step] for step in range(count)] + [theirs[step] for step in range(count)],
        scratch=[pltpu.VMEM((narrow, wide), f32)],
    )
    (late_out,) = whole_arrays(
        late_total_kernel, [shape((rows, channels), bf16)], [own_late] + late_terms
    )
    return (late_out[None], input_grad[None], grad_expand[None], grad_reduce[None])


def solution(mesh):
    in_specs = (
        P("section", "dev", None),
        P("dev", None),
        P("section", None),
        P("section", None),
        P("section", None, "dev"),
        P("section", "dev"),
        P("section", "dev"),
        P("section", "dev", None),
        P("section", "dev", None),
        P("section", "dev", None),
        P("dev", None),
        P("section", None, None),
        P("section", None, None),
    )
    out_specs = (
        P("section", "dev", None),
        P("section", "dev", None),
        P("section", None, None),
        P("section", None, None),
    )
    return jax.shard_map(shards, mesh=mesh, in_specs=in_specs, out_specs=out_specs, check_vma=False)
```

```python
import functools
import math

import jax
import jax.numpy as jnp
from jax import lax
from jax.experimental import pallas as pl
from jax.experimental.pallas import tpu as pltpu
from jax.sharding import PartitionSpec as P

epsilon = 1e-05
bf16 = jnp.bfloat16
f32 = jnp.float32


def from_behind(x, axis, by):
    peers = lax.axis_size(axis)
    pairs = [(i, i + by) for i in range(peers) if 0 <= i + by < peers]
    return lax.ppermute(x, axis, pairs)


def swap(x):
    return lax.ppermute(x, "dev", [(i, i ^ 1) for i in range(lax.axis_size("dev"))])


def partner(chip, step, count):
    return chip ^ step if count & (count - 1) == 0 else lax.rem(chip + step, count)


def across(x, step, back=False):
    count = lax.axis_size("dev") // 2
    pairs = []
    for chip in range(count):
        other = chip ^ step if count & (count - 1) == 0 else (chip + step) % count
        for core in range(2):
            here, there = 2 * chip + core, 2 * other + core
            pairs.append((there, here) if back else (here, there))
    return lax.ppermute(x, "dev", pairs)


def in_pairs(count):
    return count >= 4 and count & (count - 1) == 0


def gather(x):
    count = lax.axis_size("dev") // 2
    got = {0: x}
    if not in_pairs(count):
        for step in range(count - 1, 0, -1):
            got[step] = across(x, step, back=True)
        return got
    far = range(count - 2, 0, -2)
    for step in far:
        got[step] = across(x, step)
    got[1] = across(x, 1)
    for step in far:
        got[step ^ 1] = across(got[step], 1)
    return got


def scatter(pieces):
    count = lax.axis_size("dev") // 2
    if not in_pairs(count):
        return [across(pieces[step].astype(bf16), step) for step in range(count - 1, 0, -1)]
    far = range(count - 2, 0, -2)
    inner = {}
    for step in far:
        inner[step] = across(pieces[step ^ 1], 1)
    terms = [across(pieces[1], 1)]
    for step in far:
        both = (pieces[step].astype(f32) + inner[step].astype(f32)).astype(bf16)
        terms.append(across(both, step))
    return terms


def inner_steps(count):
    return list(range(count - 1, 2, -2)) if in_pairs(count) else []


def piece_type(step, count):
    return f32 if in_pairs(count) and step % 2 == 0 else bf16


def whole_arrays(body, outs, args, flops=0, scratch=(), mib=24):
    moved = sum(math.prod(a.shape) * a.dtype.itemsize for a in (*args, *outs))
    return pl.pallas_call(
        body,
        out_shape=list(outs),
        in_specs=[pl.BlockSpec(memory_space=pltpu.VMEM)] * len(args),
        out_specs=[pl.BlockSpec(memory_space=pltpu.VMEM)] * len(outs),
        scratch_shapes=list(scratch),
        compiler_params=pltpu.CompilerParams(vmem_limit_bytes=mib * 2**20),
        cost_estimate=pl.CostEstimate(
            flops=max(flops, moved), bytes_accessed=moved, transcendentals=0
        ),
    )(*args)


def shape(dims, dtype):
    return jax.ShapeDtypeStruct(dims, dtype)


def tile_of(extent, limit, unit):
    fitting = [t for t in range(unit, limit + 1, unit) if extent % t == 0]
    return fitting[-1] if fitting else extent


def affine(sums, squares, count, gain, shift):
    average = sums / count
    second = squares / count
    spread = gain * lax.rsqrt(second - average * average + epsilon)
    return (spread, shift - average * spread)


def silu(values):
    return values * jax.nn.sigmoid(values)


def cut_kernel(starts, whole, *refs):
    for part, ref in enumerate(refs):
        ref[...] = whole[starts[part] : starts[part + 1], :]


def early_pre_kernel(starts, saved, weight, *refs):
    parts = len(starts) - 1
    for part in range(parts):
        act, bend = refs[2 * part : 2 * part + 2]
        first, extent = starts[part], starts[part + 1] - starts[part]
        tile = tile_of(extent, 256, 16)

        @pl.loop(0, extent // tile)
        def _(index):
            here = pl.ds(pl.multiple_of(index * tile, tile), tile)
            rows = pl.ds(pl.multiple_of(first + index * tile, 16), tile)
            pre = jnp.dot(saved[rows, :], weight[...], preferred_element_type=f32)
            sigma = jax.nn.sigmoid(pre)
            act[here, :] = (pre * sigma).astype(bf16)
            bend[here, :] = (sigma * (1.0 + pre * (1.0 - sigma))).astype(bf16)

        if part:
            refs[2 * parts + part - 1][...] = saved[first : first + extent, :]


def early_grads_kernel(sections, count, first, last_part, saved, leaving, arrived, act, bend, weight, *refs):
    last = lax.axis_index("section") == sections - 1
    extent = arrived.shape[0]
    outs = 4 + len(inner_steps(count)) if last_part else 4
    before, (grad, slope, one_out, two_out, *urgent) = refs[:-outs], refs[-outs:]
    tile = tile_of(extent, 672, 16)

    @pl.loop(0, extent // tile)
    def _(index):
        rows = pl.ds(pl.multiple_of(index * tile, tile), tile)
        whole = pl.ds(pl.multiple_of(first + index * tile, 16), tile)
        here = jnp.where(last, leaving[whole, :], arrived[rows, :])
        grad[rows, :] = here
        back = lax.dot_general(
            here, weight[...], (((1,), (1,)), ((), ())), preferred_element_type=f32
        )
        slope[rows, :] = (back * bend[rows, :].astype(f32)).astype(bf16)

    over_rows = (((0,), (0,)), ((), ()))
    one = lax.dot_general(saved[:extent, :], slope[...], over_rows, preferred_element_type=f32)
    two = lax.dot_general(grad[...], act[...], over_rows, preferred_element_type=f32)
    if before:
        one, two = one + before[0][...], two + before[1][...]
    if last_part:
        first_core = lax.rem(lax.axis_index("dev"), 2) == 0
        one_out[...] = jnp.where(first_core, one, two)
        two_out[...] = jnp.where(first_core, two, one).astype(bf16)
        for step, out in zip(inner_steps(count), urgent):
            out[...] = two_out[rows_of(step, count, out.shape[0]), :]
    else:
        one_out[...] = one
        two_out[...] = two


def input_grad_kernel(parts, weight, *refs):
    out, start = refs[-1], 0
    for part in range(parts):
        grad, slope = refs[2 * part : 2 * part + 2]
        extent = grad.shape[0]
        tile = tile_of(extent, 1024, 16)
        first = start

        @pl.loop(0, extent // tile)
        def _(index):
            rows = pl.ds(pl.multiple_of(index * tile, tile), tile)
            whole = pl.ds(pl.multiple_of(first + index * tile, 16), tile)
            term = lax.dot_general(
                slope[rows, :], weight[...], (((1,), (1,)), ((), ())), preferred_element_type=f32
            )
            out[whole, :] = (grad[rows, :].astype(f32) + term).astype(bf16)

        start += extent


def rows_of(step, count, extent):
    chip = lax.div(lax.axis_index("dev"), 2)
    index = partner(chip, step, count) if step else chip
    return pl.ds(pl.multiple_of(index * extent, extent), extent)


def urgent_kernel(count, keep, *refs):
    steps = inner_steps(count)
    for step, got, out in zip(steps, refs[: len(steps)], refs[len(steps) :]):
        rows = rows_of(step, count, out.shape[0])
        out[...] = (keep[rows, :] + got[...].astype(f32)).astype(bf16)


def pieces_kernel(count, steps, keep, got, *pieces):
    for step, out in zip(steps, pieces):
        rows = rows_of(step, count, out.shape[0])
        out[...] = (keep[rows, :] + got[rows, :].astype(f32)).astype(out.dtype)


def total_kernel(factor, own, *refs):
    total = own[...]
    for got in refs[:-1]:
        total = total + got[...].astype(f32)
    refs[-1][...] = (total * factor).astype(bf16)


def assemble_kernel(count, *refs):
    mine, theirs = refs[:count], refs[count : 2 * count]
    expand, reduce, one_held, two_held, turned, done = refs[2 * count :]
    first_core = lax.rem(lax.axis_index("dev"), 2) == 0
    for step in range(count):
        here = rows_of(step, count, mine[step].shape[0])
        one, two = mine[step][...], theirs[step][...]
        one_held[here, :] = jnp.where(first_core, one, two).astype(f32)
        two_held[here, :] = jnp.where(first_core, two, one)
    copies = [pltpu.make_async_copy(one_held, expand, done.at[0])]
    copies[0].start()
    columns = reduce.shape[0]
    extent = columns // (done.shape[0] - 1)
    for index in range(columns // extent):
        here = slice(index * extent, (index + 1) * extent)
        turned[here, :] = two_held[:, here].T.astype(f32)
        copies.append(
            pltpu.make_async_copy(turned.at[here, :], reduce.at[here, :], done.at[index + 1])
        )
        copies[-1].start()
    for copy in copies:
        copy.wait()


def assemble(count, pieces, dims):
    rows, columns = dims
    extent = tile_of(columns, 256, 128)
    moved = 8 * rows * columns
    return pl.pallas_call(
        functools.partial(assemble_kernel, count),
        name="assemble",
        out_shape=[shape((rows, columns), f32), shape((columns, rows), f32)],
        in_specs=[pl.BlockSpec(memory_space=pltpu.VMEM)] * len(pieces),
        out_specs=[pl.BlockSpec(memory_space=pl.ANY)] * 2,
        scratch_shapes=[
            pltpu.VMEM((rows, columns), f32),
            pltpu.VMEM((rows, columns), bf16),
            pltpu.VMEM((columns, rows), f32),
            pltpu.SemaphoreType.DMA((1 + columns // extent,)),
        ],
        compiler_params=pltpu.CompilerParams(vmem_limit_bytes=24 * 2**20),
        cost_estimate=pl.CostEstimate(flops=moved, bytes_accessed=moved, transcendentals=0),
    )(*pieces)


def late_sums_kernel(*refs):
    sums = 0.0
    squares = 0.0
    for block in refs[:-1]:
        values = block[...].astype(f32)
        sums = sums + jnp.sum(values, axis=0, keepdims=True)
        squares = squares + jnp.sum(values * values, axis=0, keepdims=True)
    refs[-1][...] = jnp.concatenate([sums, squares], axis=0)


def late_inner_kernel(count, total_rows, *refs):
    blocks = refs[:count]
    mine, got, gain, shift, weight, weight_two, inner, sums, swapped, first = refs[count:]
    spread, offset = affine(
        mine[0:1, :] + got[0:1, :], mine[1:2, :] + got[1:2, :], total_rows, gain[...], shift[...]
    )
    used, held = blocks[0].shape[0], first.shape[0] // count
    if used < held:
        first[...] = jnp.zeros_like(first)
    for index, block in enumerate(blocks):
        values = silu(block[...].astype(f32) * spread + offset).astype(bf16)
        first[index * held : index * held + used, :] = values
    hidden = weight.shape[1]
    tile = tile_of(hidden, 256, 128)
    for part, source in enumerate((weight, weight_two)):
        for start in range(0, hidden, tile):
            term = jnp.dot(first[...], source[:, start : start + tile], preferred_element_type=f32)
            here = slice(part * hidden + start, part * hidden + start + tile)
            there = slice((1 - part) * hidden + start, (1 - part) * hidden + start + tile)
            inner[:, here] = term
            both = jnp.concatenate(
                [
                    jnp.sum(term, axis=0, keepdims=True),
                    jnp.sum(term * term, axis=0, keepdims=True),
                ],
                axis=0,
            )
            sums[:, here] = both
            swapped[:, there] = both


def late_hidden_kernel(
    count, total_rows, inner, sums, got, one, two, weight, weight_two, rows, own, *refs
):
    partials, hidden = refs[:-1], refs[-1]
    extent = weight.shape[0]
    for part, gain_shift in enumerate((one, two)):
        here = slice(part * extent, (part + 1) * extent)
        spread, offset = affine(
            sums[0:1, here] + got[0:1, here],
            sums[1:2, here] + got[1:2, here],
            total_rows,
            gain_shift[0:1, :],
            gain_shift[1:2, :],
        )
        hidden[:, here] = silu(inner[:, here] * spread + offset).astype(bf16)
    used, held = rows.shape[0], inner.shape[0] // count
    tile = tile_of(weight.shape[1], 256, 128)
    for start in range(0, weight.shape[1], tile):
        columns = slice(start, start + tile)
        term = jnp.dot(hidden[:, :extent], weight[:, columns], preferred_element_type=f32)
        term = term + jnp.dot(
            hidden[:, extent:], weight_two[:, columns], preferred_element_type=f32
        )
        own[:, columns] = rows[:, columns].astype(f32) + term[:used]
        for step in range(1, count):
            out = partials[step - 1]
            out[:, columns] = term[step * held : step * held + used].astype(out.dtype)


def late_total_kernel(own, *refs):
    total = own[...]
    for got in refs[:-1]:
        total = total + got[...].astype(f32)
    refs[-1][...] = total.astype(bf16)


def shards(
    late_sent,
    entry_rows,
    gain_first,
    shift_first,
    expand_late,
    gain_inner,
    shift_inner,
    reduce_late,
    early_saved,
    upstream_grad,
    exit_grad,
    expand_early,
    reduce_early,
):
    sections, count = lax.axis_size("section"), lax.axis_size("dev") // 2
    section = lax.axis_index("section")
    steps = range(1, count)

    late_arrived = from_behind(late_sent[0], "section", 1)
    pixels = upstream_grad.shape[1]
    tail = 2 * tile_of(pixels, 256, 16)
    starts = (0, pixels - tail, pixels) if tail < pixels else (0, pixels)
    parts = len(starts) - 1
    extents = [starts[part + 1] - starts[part] for part in range(parts)]
    leaving = whole_arrays(
        functools.partial(cut_kernel, starts),
        [shape((extent, upstream_grad.shape[2]), bf16) for extent in extents],
        [upstream_grad[0]],
    )
    early_arrived = []
    for part in range(parts):
        early_arrived.append(from_behind(leaving[part], "section", -1))
    expand_two, reduce_two = swap(expand_late[0]), swap(reduce_late[0])
    one = jnp.concatenate([gain_inner, shift_inner], axis=0)
    two = swap(one)

    own_rows = jnp.where(section == 0, entry_rows, late_arrived)
    blocks = gather(own_rows)

    saved = early_saved[0]
    narrow, wide = expand_early.shape[1:]
    work = 2 * narrow * wide
    pre = whole_arrays(
        functools.partial(early_pre_kernel, starts),
        [shape((extents[part // 2], wide), bf16) for part in range(2 * parts)]
        + [shape((extent, narrow), bf16) for extent in extents[1:]],
        [saved, expand_early[0]],
        pixels * work,
    )
    share = narrow // count
    urgent_steps = inner_steps(count)
    grads, sums_so_far = [], []
    for part in range(parts):
        final = part == parts - 1
        grad, slope, keep, send, *urgent = whole_arrays(
            functools.partial(early_grads_kernel, sections, count, starts[part], final),
            [
                shape((extents[part], narrow), bf16),
                shape((extents[part], wide), bf16),
                shape((narrow, wide), f32),
                shape((narrow, wide), bf16 if final else f32),
            ]
            + [shape((share, wide), bf16)] * (len(urgent_steps) if final else 0),
            [
                pre[2 * parts + part - 1] if part else saved,
                exit_grad,
                early_arrived[part],
                *pre[2 * part : 2 * part + 2],
                reduce_early[0],
                *sums_so_far,
            ],
            3 * extents[part] * work,
        )
        grads += [grad, slope]
        sums_so_far = [keep, send]
    shares = {}
    if urgent_steps:
        got_urgent = [swap(piece) for piece in urgent]
        added = whole_arrays(
            functools.partial(urgent_kernel, count),
            [shape((share, wide), bf16)] * len(urgent),
            [keep, *got_urgent],
        )
        shares.update(zip(urgent_steps, added))
    got = swap(send)
    other_steps = [step for step in range(count) if step not in shares]
    added = whole_arrays(
        functools.partial(pieces_kernel, count, other_steps),
        [shape((share, wide), piece_type(step, count) if step else f32) for step in other_steps],
        [keep, got],
    )
    shares.update(zip(other_steps, added))
    own_share = shares[0]
    terms = scatter(shares)

    rows, channels = own_rows.shape
    total_rows = rows * lax.axis_size("dev")
    held = -(-rows // 16) * 16
    hidden = expand_late.shape[2]
    late_work = 4 * count * held * channels * hidden
    listed = [blocks[step] for step in range(count)]
    (mine,) = whole_arrays(late_sums_kernel, [shape((2, channels), f32)], listed)
    others = swap(mine)
    inner, sums, swapped = whole_arrays(
        functools.partial(late_inner_kernel, count, total_rows),
        [shape((count * held, 2 * hidden), f32), shape((2, 2 * hidden), f32), shape((2, 2 * hidden), f32)],
        listed + [mine, others, gain_first, shift_first, expand_late[0], expand_two],
        late_work,
        [pltpu.VMEM((count * held, channels), bf16)],
    )
    got_sums = swap(swapped)
    own_late, *partials = whole_arrays(
        functools.partial(late_hidden_kernel, count, total_rows),
        [shape((rows, channels), f32)]
        + [shape((rows, channels), piece_type(step, count)) for step in steps],
        [inner, sums, got_sums, one, two, reduce_late[0], reduce_two, own_rows],
        late_work,
        [pltpu.VMEM((count * held, 2 * hidden), bf16)],
    )
    late_terms = scatter(dict(zip(steps, partials)))

    factor = 1.0 / math.sqrt(pixels * lax.axis_size("dev"))
    (summed,) = whole_arrays(
        functools.partial(total_kernel, factor), [shape((share, wide), bf16)], [own_share] + terms
    )
    gathered = gather(summed)
    theirs = {step: swap(gathered[step]) for step in gathered}
    (input_grad,) = whole_arrays(
        functools.partial(input_grad_kernel, parts),
        [shape((pixels, narrow), bf16)],
        [expand_early[0], *grads],
        pixels * work,
    )
    grad_expand, grad_reduce = assemble(
        count,
        [gathered[step] for step in range(count)] + [theirs[step] for step in range(count)],
        (narrow, wide),
    )
    (late_out,) = whole_arrays(
        late_total_kernel, [shape((rows, channels), bf16)], [own_late] + late_terms
    )
    return (late_out[None], input_grad[None], grad_expand[None], grad_reduce[None])


def solution(mesh):
    in_specs = (
        P("section", "dev", None),
        P("dev", None),
        P("section", None),
        P("section", None),
        P("section", None, "dev"),
        P("section", "dev"),
        P("section", "dev"),
        P("section", "dev", None),
        P("section", "dev", None),
        P("section", "dev", None),
        P("dev", None),
        P("section", None, None),
        P("section", None, None),
    )
    out_specs = (
        P("section", "dev", None),
        P("section", "dev", None),
        P("section", None, None),
        P("section", None, None),
    )
    return jax.shard_map(shards, mesh=mesh, in_specs=in_specs, out_specs=out_specs, check_vma=False)
```

```python
import functools
import math

import jax
import jax.numpy as jnp
from jax import lax
from jax.experimental import pallas as pl
from jax.experimental.pallas import tpu as pltpu
from jax.sharding import PartitionSpec as P

epsilon = 1e-05
bf16 = jnp.bfloat16
f32 = jnp.float32


def from_behind(x, axis, by):
    peers = lax.axis_size(axis)
    pairs = [(i, i + by) for i in range(peers) if 0 <= i + by < peers]
    return lax.ppermute(x, axis, pairs)


def swap(x):
    return lax.ppermute(x, "dev", [(i, i ^ 1) for i in range(lax.axis_size("dev"))])


def partner(chip, step, count):
    return chip ^ step if count & (count - 1) == 0 else lax.rem(chip + step, count)


def across(x, step, back=False):
    count = lax.axis_size("dev") // 2
    pairs = []
    for chip in range(count):
        other = chip ^ step if count & (count - 1) == 0 else (chip + step) % count
        for core in range(2):
            here, there = 2 * chip + core, 2 * other + core
            pairs.append((there, here) if back else (here, there))
    return lax.ppermute(x, "dev", pairs)


def in_pairs(count):
    return count >= 4 and count & (count - 1) == 0


def gather(x):
    count = lax.axis_size("dev") // 2
    got = {0: x}
    if not in_pairs(count):
        for step in range(count - 1, 0, -1):
            got[step] = across(x, step, back=True)
        return got
    far = range(count - 2, 0, -2)
    for step in far:
        got[step] = across(x, step)
    got[1] = across(x, 1)
    for step in far:
        got[step ^ 1] = across(got[step], 1)
    return got


def scatter(pieces, far=None):
    count = lax.axis_size("dev") // 2
    if not in_pairs(count):
        return [across(pieces[step].astype(bf16), step) for step in range(count - 1, 0, -1)]
    far = far or range(count - 2, 0, -2)
    inner = {}
    for step in far:
        inner[step] = across(pieces[step ^ 1], 1)
    terms = [across(pieces[1], 1)]
    for step in far:
        both = (pieces[step].astype(f32) + inner[step].astype(f32)).astype(bf16)
        terms.append(across(both, step))
    return terms


def inner_steps(count):
    return list(range(count - 1, 2, -2)) if in_pairs(count) else []


def piece_type(step, count):
    return f32 if in_pairs(count) and step % 2 == 0 else bf16


def whole_arrays(body, outs, args, flops=0, scratch=(), mib=24):
    moved = sum(math.prod(a.shape) * a.dtype.itemsize for a in (*args, *outs))
    return pl.pallas_call(
        body,
        out_shape=list(outs),
        in_specs=[pl.BlockSpec(memory_space=pltpu.VMEM)] * len(args),
        out_specs=[pl.BlockSpec(memory_space=pltpu.VMEM)] * len(outs),
        scratch_shapes=list(scratch),
        compiler_params=pltpu.CompilerParams(vmem_limit_bytes=mib * 2**20),
        cost_estimate=pl.CostEstimate(
            flops=max(flops, moved), bytes_accessed=moved, transcendentals=0
        ),
    )(*args)


def shape(dims, dtype):
    return jax.ShapeDtypeStruct(dims, dtype)


def tile_of(extent, limit, unit):
    fitting = [t for t in range(unit, limit + 1, unit) if extent % t == 0]
    return fitting[-1] if fitting else extent


def affine(sums, squares, count, gain, shift):
    average = sums / count
    second = squares / count
    spread = gain * lax.rsqrt(second - average * average + epsilon)
    return (spread, shift - average * spread)


def silu(values):
    return values * jax.nn.sigmoid(values)


def cut_kernel(starts, whole, *refs):
    for part, ref in enumerate(refs):
        ref[...] = whole[starts[part] : starts[part + 1], :]


def early_pre_kernel(starts, saved, weight, *refs):
    parts = len(starts) - 1
    for part in range(parts):
        act, bend = refs[2 * part : 2 * part + 2]
        first, extent = starts[part], starts[part + 1] - starts[part]
        tile = tile_of(extent, 256, 16)

        @pl.loop(0, extent // tile)
        def _(index):
            here = pl.ds(pl.multiple_of(index * tile, tile), tile)
            rows = pl.ds(pl.multiple_of(first + index * tile, 16), tile)
            pre = jnp.dot(saved[rows, :], weight[...], preferred_element_type=f32)
            sigma = jax.nn.sigmoid(pre)
            act[here, :] = (pre * sigma).astype(bf16)
            bend[here, :] = (sigma * (1.0 + pre * (1.0 - sigma))).astype(bf16)

        if part:
            refs[2 * parts + part - 1][...] = saved[first : first + extent, :]


def early_grads_kernel(sections, count, first, last_part, saved, leaving, arrived, act, bend, weight, *refs):
    last = lax.axis_index("section") == sections - 1
    extent = arrived.shape[0]
    outs = 4 + len(inner_steps(count)) if last_part else 4
    before, (grad, slope, one_out, two_out, *urgent) = refs[:-outs], refs[-outs:]
    tile = tile_of(extent, 672, 16)

    @pl.loop(0, extent // tile)
    def _(index):
        rows = pl.ds(pl.multiple_of(index * tile, tile), tile)
        whole = pl.ds(pl.multiple_of(first + index * tile, 16), tile)
        here = jnp.where(last, leaving[whole, :], arrived[rows, :])
        grad[rows, :] = here
        back = lax.dot_general(
            here, weight[...], (((1,), (1,)), ((), ())), preferred_element_type=f32
        )
        slope[rows, :] = (back * bend[rows, :].astype(f32)).astype(bf16)

    over_rows = (((0,), (0,)), ((), ()))
    one = lax.dot_general(saved[:extent, :], slope[...], over_rows, preferred_element_type=f32)
    two = lax.dot_general(grad[...], act[...], over_rows, preferred_element_type=f32)
    if before:
        one, two = one + before[0][...], two + before[1][...]
    if last_part:
        first_core = lax.rem(lax.axis_index("dev"), 2) == 0
        one_out[...] = jnp.where(first_core, one, two)
        two_out[...] = jnp.where(first_core, two, one).astype(bf16)
        for step, out in zip(inner_steps(count), urgent):
            out[...] = two_out[rows_of(step, count, out.shape[0]), :]
    else:
        one_out[...] = one
        two_out[...] = two


def input_grad_kernel(parts, weight, *refs):
    out, start = refs[-1], 0
    for part in range(parts):
        grad, slope = refs[2 * part : 2 * part + 2]
        extent = grad.shape[0]
        tile = tile_of(extent, 1024, 16)
        first = start

        @pl.loop(0, extent // tile)
        def _(index):
            rows = pl.ds(pl.multiple_of(index * tile, tile), tile)
            whole = pl.ds(pl.multiple_of(first + index * tile, 16), tile)
            term = lax.dot_general(
                slope[rows, :], weight[...], (((1,), (1,)), ((), ())), preferred_element_type=f32
            )
            out[whole, :] = (grad[rows, :].astype(f32) + term).astype(bf16)

        start += extent


def rows_of(step, count, extent):
    chip = lax.div(lax.axis_index("dev"), 2)
    index = partner(chip, step, count) if step else chip
    return pl.ds(pl.multiple_of(index * extent, extent), extent)


def urgent_kernel(count, keep, *refs):
    steps = inner_steps(count)
    for step, got, out in zip(steps, refs[: len(steps)], refs[len(steps) :]):
        rows = rows_of(step, count, out.shape[0])
        out[...] = (keep[rows, :] + got[...].astype(f32)).astype(bf16)


def pieces_kernel(count, steps, keep, got, *pieces):
    for step, out in zip(steps, pieces):
        rows = rows_of(step, count, out.shape[0])
        out[...] = (keep[rows, :] + got[rows, :].astype(f32)).astype(out.dtype)


def total_kernel(factor, own, *refs):
    total = own[...]
    for got in refs[:-1]:
        total = total + got[...].astype(f32)
    refs[-1][...] = (total * factor).astype(bf16)


def assemble_kernel(count, *refs):
    mine, theirs = refs[:count], refs[count : 2 * count]
    expand, reduce, one_held, two_held, turned, done = refs[2 * count :]
    first_core = lax.rem(lax.axis_index("dev"), 2) == 0
    for step in range(count):
        here = rows_of(step, count, mine[step].shape[0])
        one, two = mine[step][...], theirs[step][...]
        one_held[here, :] = jnp.where(first_core, one, two).astype(f32)
        two_held[here, :] = jnp.where(first_core, two, one)
    copies = [pltpu.make_async_copy(one_held, expand, done.at[0])]
    copies[0].start()
    columns = reduce.shape[0]
    extent = columns // (done.shape[0] - 1)
    for index in range(columns // extent):
        here = slice(index * extent, (index + 1) * extent)
        turned[here, :] = two_held[:, here].T.astype(f32)
        copies.append(
            pltpu.make_async_copy(turned.at[here, :], reduce.at[here, :], done.at[index + 1])
        )
        copies[-1].start()
    for copy in copies:
        copy.wait()


def assemble(count, pieces, dims):
    rows, columns = dims
    extent = tile_of(columns, 256, 128)
    moved = 8 * rows * columns
    return pl.pallas_call(
        functools.partial(assemble_kernel, count),
        name="assemble",
        out_shape=[shape((rows, columns), f32), shape((columns, rows), f32)],
        in_specs=[pl.BlockSpec(memory_space=pltpu.VMEM)] * len(pieces),
        out_specs=[pl.BlockSpec(memory_space=pl.ANY)] * 2,
        scratch_shapes=[
            pltpu.VMEM((rows, columns), f32),
            pltpu.VMEM((rows, columns), bf16),
            pltpu.VMEM((columns, rows), f32),
            pltpu.SemaphoreType.DMA((1 + columns // extent,)),
        ],
        compiler_params=pltpu.CompilerParams(vmem_limit_bytes=24 * 2**20),
        cost_estimate=pl.CostEstimate(flops=moved, bytes_accessed=moved, transcendentals=0),
    )(*pieces)


def late_sums_kernel(*refs):
    sums = 0.0
    squares = 0.0
    for block in refs[:-1]:
        values = block[...].astype(f32)
        sums = sums + jnp.sum(values, axis=0, keepdims=True)
        squares = squares + jnp.sum(values * values, axis=0, keepdims=True)
    refs[-1][...] = jnp.concatenate([sums, squares], axis=0)


def late_inner_kernel(count, total_rows, *refs):
    blocks = refs[:count]
    mine, got, gain, shift, weight, weight_two, inner, sums, swapped, first = refs[count:]
    spread, offset = affine(
        mine[0:1, :] + got[0:1, :], mine[1:2, :] + got[1:2, :], total_rows, gain[...], shift[...]
    )
    used, held = blocks[0].shape[0], first.shape[0] // count
    if used < held:
        first[...] = jnp.zeros_like(first)
    for index, block in enumerate(blocks):
        values = silu(block[...].astype(f32) * spread + offset).astype(bf16)
        first[index * held : index * held + used, :] = values
    hidden = weight.shape[1]
    tile = tile_of(hidden, 256, 128)
    for part, source in enumerate((weight, weight_two)):
        for start in range(0, hidden, tile):
            term = jnp.dot(first[...], source[:, start : start + tile], preferred_element_type=f32)
            here = slice(part * hidden + start, part * hidden + start + tile)
            there = slice((1 - part) * hidden + start, (1 - part) * hidden + start + tile)
            inner[:, here] = term
            both = jnp.concatenate(
                [
                    jnp.sum(term, axis=0, keepdims=True),
                    jnp.sum(term * term, axis=0, keepdims=True),
                ],
                axis=0,
            )
            sums[:, here] = both
            swapped[:, there] = both


def late_hidden_kernel(
    count, total_rows, inner, sums, got, one, two, weight, weight_two, rows, own, *refs
):
    partials, hidden = refs[:-1], refs[-1]
    extent = weight.shape[0]
    for part, gain_shift in enumerate((one, two)):
        here = slice(part * extent, (part + 1) * extent)
        spread, offset = affine(
            sums[0:1, here] + got[0:1, here],
            sums[1:2, here] + got[1:2, here],
            total_rows,
            gain_shift[0:1, :],
            gain_shift[1:2, :],
        )
        hidden[:, here] = silu(inner[:, here] * spread + offset).astype(bf16)
    used, held = rows.shape[0], inner.shape[0] // count
    tile = tile_of(weight.shape[1], 256, 128)
    for start in range(0, weight.shape[1], tile):
        columns = slice(start, start + tile)
        term = jnp.dot(hidden[:, :extent], weight[:, columns], preferred_element_type=f32)
        term = term + jnp.dot(
            hidden[:, extent:], weight_two[:, columns], preferred_element_type=f32
        )
        own[:, columns] = rows[:, columns].astype(f32) + term[:used]
        for step in range(1, count):
            out = partials[step - 1]
            out[:, columns] = term[step * held : step * held + used].astype(out.dtype)


def late_total_kernel(own, *refs):
    total = own[...]
    for got in refs[:-1]:
        total = total + got[...].astype(f32)
    refs[-1][...] = total.astype(bf16)


def shards(
    late_sent,
    entry_rows,
    gain_first,
    shift_first,
    expand_late,
    gain_inner,
    shift_inner,
    reduce_late,
    early_saved,
    upstream_grad,
    exit_grad,
    expand_early,
    reduce_early,
):
    sections, count = lax.axis_size("section"), lax.axis_size("dev") // 2
    section = lax.axis_index("section")
    steps = range(1, count)

    late_arrived = from_behind(late_sent[0], "section", 1)
    pixels = upstream_grad.shape[1]
    tail = 2 * tile_of(pixels, 256, 16)
    starts = (0, pixels - tail, pixels) if tail < pixels else (0, pixels)
    parts = len(starts) - 1
    extents = [starts[part + 1] - starts[part] for part in range(parts)]
    leaving = whole_arrays(
        functools.partial(cut_kernel, starts),
        [shape((extent, upstream_grad.shape[2]), bf16) for extent in extents],
        [upstream_grad[0]],
    )
    early_arrived = []
    for part in range(parts):
        early_arrived.append(from_behind(leaving[part], "section", -1))
    expand_two, reduce_two = swap(expand_late[0]), swap(reduce_late[0])
    one = jnp.concatenate([gain_inner, shift_inner], axis=0)
    two = swap(one)

    own_rows = jnp.where(section == 0, entry_rows, late_arrived)
    blocks = gather(own_rows)

    saved = early_saved[0]
    narrow, wide = expand_early.shape[1:]
    work = 2 * narrow * wide
    pre = whole_arrays(
        functools.partial(early_pre_kernel, starts),
        [shape((extents[part // 2], wide), bf16) for part in range(2 * parts)]
        + [shape((extent, narrow), bf16) for extent in extents[1:]],
        [saved, expand_early[0]],
        pixels * work,
    )
    share = narrow // count
    urgent_steps = inner_steps(count)
    grads, sums_so_far = [], []
    for part in range(parts):
        final = part == parts - 1
        grad, slope, keep, send, *urgent = whole_arrays(
            functools.partial(early_grads_kernel, sections, count, starts[part], final),
            [
                shape((extents[part], narrow), bf16),
                shape((extents[part], wide), bf16),
                shape((narrow, wide), f32),
                shape((narrow, wide), bf16 if final else f32),
            ]
            + [shape((share, wide), bf16)] * (len(urgent_steps) if final else 0),
            [
                pre[2 * parts + part - 1] if part else saved,
                exit_grad,
                early_arrived[part],
                *pre[2 * part : 2 * part + 2],
                reduce_early[0],
                *sums_so_far,
            ],
            3 * extents[part] * work,
        )
        grads += [grad, slope]
        sums_so_far = [keep, send]
    shares = {}
    if urgent_steps:
        got_urgent = [swap(piece) for piece in urgent]
        added = whole_arrays(
            functools.partial(urgent_kernel, count),
            [shape((share, wide), bf16)] * len(urgent),
            [keep, *got_urgent],
        )
        shares.update(zip(urgent_steps, added))
    got = swap(send)
    other_steps = [step for step in range(count) if step not in shares]
    added = whole_arrays(
        functools.partial(pieces_kernel, count, other_steps),
        [shape((share, wide), piece_type(step, count) if step else f32) for step in other_steps],
        [keep, got],
    )
    shares.update(zip(other_steps, added))
    own_share = shares[0]
    terms = scatter(shares)

    rows, channels = own_rows.shape
    total_rows = rows * lax.axis_size("dev")
    held = -(-rows // 16) * 16
    hidden = expand_late.shape[2]
    late_work = 4 * count * held * channels * hidden
    listed = [blocks[step] for step in range(count)]
    (mine,) = whole_arrays(late_sums_kernel, [shape((2, channels), f32)], listed)
    others = swap(mine)
    inner, sums, swapped = whole_arrays(
        functools.partial(late_inner_kernel, count, total_rows),
        [shape((count * held, 2 * hidden), f32), shape((2, 2 * hidden), f32), shape((2, 2 * hidden), f32)],
        listed + [mine, others, gain_first, shift_first, expand_late[0], expand_two],
        late_work,
        [pltpu.VMEM((count * held, channels), bf16)],
    )
    got_sums = swap(swapped)
    own_late, *partials = whole_arrays(
        functools.partial(late_hidden_kernel, count, total_rows),
        [shape((rows, channels), f32)]
        + [
            shape((rows, channels), f32 if step > 1 and step % 2 else bf16) for step in steps
        ],
        [inner, sums, got_sums, one, two, reduce_late[0], reduce_two, own_rows],
        late_work,
        [pltpu.VMEM((count * held, 2 * hidden), bf16)],
    )
    late_terms = scatter(dict(zip(steps, partials)), range(count - 1, 2, -2))

    factor = 1.0 / math.sqrt(pixels * lax.axis_size("dev"))
    (summed,) = whole_arrays(
        functools.partial(total_kernel, factor), [shape((share, wide), bf16)], [own_share] + terms
    )
    gathered = gather(summed)
    theirs = {step: swap(gathered[step]) for step in gathered}
    (input_grad,) = whole_arrays(
        functools.partial(input_grad_kernel, parts),
        [shape((pixels, narrow), bf16)],
        [expand_early[0], *grads],
        pixels * work,
    )
    grad_expand, grad_reduce = assemble(
        count,
        [gathered[step] for step in range(count)] + [theirs[step] for step in range(count)],
        (narrow, wide),
    )
    (late_out,) = whole_arrays(
        late_total_kernel, [shape((rows, channels), bf16)], [own_late] + late_terms
    )
    return (late_out[None], input_grad[None], grad_expand[None], grad_reduce[None])


def solution(mesh):
    in_specs = (
        P("section", "dev", None),
        P("dev", None),
        P("section", None),
        P("section", None),
        P("section", None, "dev"),
        P("section", "dev"),
        P("section", "dev"),
        P("section", "dev", None),
        P("section", "dev", None),
        P("section", "dev", None),
        P("dev", None),
        P("section", None, None),
        P("section", None, None),
    )
    out_specs = (
        P("section", "dev", None),
        P("section", "dev", None),
        P("section", None, None),
        P("section", None, None),
    )
    return jax.shard_map(shards, mesh=mesh, in_specs=in_specs, out_specs=out_specs, check_vma=False)
```
